512 devices in a mesh: dp: 64 (over y, x, z_lo), feat: 8 (over z_hi, core).
Axes of the slice: x: 4, y: 8, z: 8 (z_hi: 4, z_lo: 2; z = z_hi * 2 + z_lo), core: 2. Of those that a mesh axis runs over, the one named last changes fastest.
Arguments:
- embeddings: bfloat16 [327680, 2048], P('dp', 'feat'), may hold values from -80 to 80
- slot_image: int32 [327680], P('dp'), may hold values from 0 to 32767, as said below
- slot_view: int32 [327680], P('dp'), may hold values from 0 to 10, as said below
- pair_table: int32 [2, 2], replicated, may hold values from 0 to 9, as said below
Outputs:
- correlation: float32 [2, 2048, 2048], P(None, 'feat', 'dp')
The draws below stay inside these ranges and needn't reach their ends.
Inputs may be any that keep to these rules, and one draw needn't show every extreme that they name: `slot_image`: image ids of dp index d run from d * 512 to (d + 1) * 512 - 1. Each image has views 0 and 1 and local views 2 to 1 + k with k from 1 to 8; the first image of every dp index has all 10 views; every (image, view) stands in one slot at most; empty slots name an image of their own dp index. `slot_view`: empty slots carry view 10 and come after the used slots of their dp index; the last dp index fills all its slots. `pair_table`: each pair's first view is global (0 or 1) and its second view differs from it.
All inputs are finite; a program needn't handle non-finite values.
Results may differ from the reference program's by a relative error of at most 0.00035.
Values may be sent and summed in bfloat16 or wider, within the bound.
A program may use at most 64 MiB of HBM per device.

```python
import jax
import jax.numpy as jnp
from jax import lax

WIN = 2048
IMG_DEV = 512
LOCALS = 8
PAIRS = 2
VIEWS = 10
ROWS_DEV = 5120
IMAGES = 32768
TOTAL_ROWS = 327680


def crop_lists(key):
    device_count = IMAGES // IMG_DEV
    first_key, second_key = jax.random.split(key)
    device_index = jnp.arange(device_count, dtype=jnp.int32)[:, None]
    upper_bound = 1 + 7 * device_index // max(device_count - 1, 1)
    raw_bits = jax.random.randint(first_key, (device_count, IMG_DEV), 0, 1 << 20)
    local_counts = raw_bits % upper_bound + 1
    local_counts = jnp.where(device_index == device_count - 1, LOCALS, local_counts)
    local_counts = local_counts.at[:, 0].set(LOCALS)
    view_grid = jnp.arange(VIEWS, dtype=jnp.int32)[None, None, :]
    usable = (view_grid < 2 + local_counts[:, :, None]).reshape(device_count, ROWS_DEV)
    device_keys = jax.random.split(second_key, device_count)
    shuffled = jax.vmap(lambda one_key: jax.random.permutation(one_key, ROWS_DEV))(device_keys).astype(jnp.int32)
    sort_score = jnp.where(usable, shuffled, ROWS_DEV + jnp.arange(ROWS_DEV, dtype=jnp.int32)[None, :])
    sorted_slots = jnp.argsort(sort_score, axis=1, stable=True).astype(jnp.int32)
    usable_sorted = jnp.take_along_axis(usable, sorted_slots, axis=1)
    image_ids = device_index * IMG_DEV + sorted_slots // VIEWS
    view_ids = jnp.where(usable_sorted, sorted_slots % VIEWS, VIEWS)
    return (image_ids.reshape(-1).astype(jnp.int32), view_ids.reshape(-1).astype(jnp.int32))


def draw_slot_image(key, part):
    return crop_lists(jax.random.fold_in(key, 11))[0]


def draw_slot_view(key, part):
    return crop_lists(jax.random.fold_in(key, 11))[1]


def draw_pair_table(key, part):
    first_key, second_key, third_key = jax.random.split(jax.random.fold_in(key, 13), 3)
    global_view = jax.random.randint(first_key, (PAIRS,), 0, 2)
    other_view = (global_view + 1 + jax.random.randint(second_key, (PAIRS,), 0, VIEWS - 1)) % VIEWS
    chosen = jax.random.randint(third_key, (), 0, PAIRS)
    is_chosen = jnp.arange(PAIRS, dtype=jnp.int32) == chosen
    global_view = jnp.where(is_chosen, 0, global_view)
    other_view = jnp.where(is_chosen, VIEWS - 1, other_view)
    return jnp.stack([global_view, other_view], axis=1).astype(jnp.int32)


def draw_embeddings(key, part):
    image_ids, view_ids = crop_lists(jax.random.fold_in(key, 11))
    base_key = jax.random.fold_in(key, 12)
    latent_key, noise_key, column_key = jax.random.split(base_key, 3)
    latent = jax.random.truncated_normal(latent_key, -4.0, 4.0, (IMAGES, WIN), jnp.float32)
    column_scale = jnp.exp(jax.random.uniform(column_key, (WIN,), jnp.float32, jnp.log(0.5), jnp.log(5.0)))
    noise = jax.random.truncated_normal(noise_key, -4.0, 4.0, (TOTAL_ROWS, WIN), jnp.float32)
    values = (jnp.take(latent, image_ids, axis=0) + 0.6 * noise) * column_scale
    return values.astype(jnp.bfloat16)


def setup_inputs(seed: int = 0) -> dict:
    key_of = jax.random.split(jax.random.key(seed), 5)
    embeddings = draw_embeddings(jax.random.fold_in(key_of[4], 71), 0)
    slot_image = draw_slot_image(jax.random.fold_in(key_of[4], 71), 0)
    slot_view = draw_slot_view(jax.random.fold_in(key_of[4], 71), 0)
    pair_table = draw_pair_table(jax.random.fold_in(key_of[4], 71), 0)
    return {"embeddings": embeddings, "slot_image": slot_image, "slot_view": slot_view, "pair_table": pair_table}


EPS = 1e-05

def locate(slot_image, slot_view, view_id):
    positions = jnp.arange(slot_view.shape[0], dtype=jnp.int32) + 1
    marked = jnp.where(slot_view == view_id, positions, jnp.zeros((), jnp.int32))
    return jnp.zeros((IMAGES,), jnp.int32).at[slot_image].max(marked) - 1

def pick_rows(embeddings, slots, present):
    taken = jnp.take(embeddings, jnp.maximum(slots, 0).astype(jnp.int32), axis=0)
    return jnp.where(present[:, None], taken, jnp.zeros((), embeddings.dtype))

def reference(embeddings, slot_image, slot_view, pair_table):
    outputs = []
    for pair_index in range(PAIRS):
        first = locate(slot_image, slot_view, pair_table[pair_index, 0])
        second = locate(slot_image, slot_view, pair_table[pair_index, 1])
        present = (first >= 0) & (second >= 0)
        first_rows = pick_rows(embeddings, first, present)
        second_rows = pick_rows(embeddings, second, present)
        total = jnp.sum(present.astype(jnp.float32))
        first_wide = first_rows.astype(jnp.float32)
        second_wide = second_rows.astype(jnp.float32)
        mean_first = lax.optimization_barrier(jnp.sum(first_wide, axis=0)) / total
        mean_second = lax.optimization_barrier(jnp.sum(second_wide, axis=0)) / total
        square_first = lax.optimization_barrier(jnp.sum(first_wide * first_wide, axis=0)) / total
        square_second = lax.optimization_barrier(jnp.sum(second_wide * second_wide, axis=0)) / total
        spread_first = jnp.sqrt(square_first - mean_first * mean_first + EPS)
        spread_second = jnp.sqrt(square_second - mean_second * mean_second + EPS)
        cross = jnp.dot(first_rows.T, second_rows, preferred_element_type=jnp.float32)
        block = (cross / total - mean_first[:, None] * mean_second[None, :]) / (spread_first[:, None] * spread_second[None, :])
        outputs.append(block)
    return jnp.stack(outputs, axis=0)
```

```python
import jax
import jax.numpy as jnp
from jax import lax
from jax.experimental import pallas as pl
from jax.experimental.pallas import tpu as pltpu
from jax.sharding import Mesh
from jax.sharding import PartitionSpec as P

WIN = 2048
IMG_DEV = 512
PAIRS = 2
WIDTH = 256
OWN = 32
NX, NY = 4, 8
BLOCK = 64
STAT = 8
ROWS = BLOCK + STAT
PART = OWN + STAT
CUT = 40
SLOTS = 1024
VIEW_STRIDE = 16
AXES = ("y", "x", "zl", "zh", "core")
FEAT = ("zh", "core")
DP = ("y", "x", "zl")
EPS = 1e-05
F32 = jnp.float32
BF16 = jnp.bfloat16
MESH = pl.DeviceIdType.MESH


def select_kernel(pair_ref, image_ref, view_ref, emb_ref, x1_ref, x2_ref, stat_ref, acc, found):
    step = pl.program_id(0)

    @pl.when(step == 0)
    def _():
        acc[...] = jnp.zeros_like(acc)
        found[...] = jnp.zeros_like(found)

    base = lax.axis_index(DP) * IMG_DEV
    key = image_ref[...] * VIEW_STRIDE + view_ref[...]
    wanted = (lax.broadcasted_iota(jnp.int32, (IMG_DEV, 128), 0) + base) * VIEW_STRIDE
    for pair in range(PAIRS):
        for side in range(2):
            target = wanted + pair_ref[pair, side]
            hits = [
                jnp.where(key[row : row + 1, :] == target, 1.0, 0.0) for row in range(SLOTS // 128)
            ]
            chosen = jnp.concatenate([hit.astype(BF16) for hit in hits], axis=1)
            acc[2 * pair + side] += jnp.dot(chosen, emb_ref[...], preferred_element_type=F32)
            if side == 1:
                found[pair] += sum(hits[1:], hits[0])

    @pl.when(step == pl.num_programs(0) - 1)
    def _():
        row = lax.broadcasted_iota(jnp.int32, (STAT, WIDTH), 0)
        for pair in range(PAIRS):
            present = jnp.sum(found[pair], axis=1, keepdims=True)
            x1_ref[pair] = jnp.where(present > 0.5, acc[2 * pair], 0.0).astype(BF16)
            second = acc[2 * pair + 1]
            x2_ref[pair] = second.T.astype(BF16)
            total = jnp.sum(second, axis=0, keepdims=True)
            square = jnp.sum(second * second, axis=0, keepdims=True)
            count = jnp.sum(present)
            stat_ref[pair] = jnp.where(
                row == 2, total, jnp.where(row == 3, square, jnp.where(row == 4, count, 0.0))
            )


def select(pair_table, slot_image, slot_view, embeddings):
    slots = embeddings.shape[0]
    steps = slots // SLOTS
    ids = pl.BlockSpec((SLOTS // 128, 128), lambda k: (k, 0))
    whole = lambda *shape: pl.BlockSpec(shape, lambda k: (0,) * len(shape))
    return pl.pallas_call(
        select_kernel,
        grid=(steps,),
        out_shape=(
            jax.ShapeDtypeStruct((PAIRS, IMG_DEV, WIDTH), BF16),
            jax.ShapeDtypeStruct((PAIRS, WIDTH, IMG_DEV), BF16),
            jax.ShapeDtypeStruct((PAIRS, STAT, WIDTH), F32),
        ),
        in_specs=[
            pl.BlockSpec(memory_space=pltpu.SMEM),
            ids,
            ids,
            pl.BlockSpec((SLOTS, WIDTH), lambda k: (k, 0)),
        ],
        out_specs=(
            whole(PAIRS, IMG_DEV, WIDTH),
            whole(PAIRS, WIDTH, IMG_DEV),
            whole(PAIRS, STAT, WIDTH),
        ),
        scratch_shapes=[
            pltpu.VMEM((2 * PAIRS, IMG_DEV, WIDTH), F32),
            pltpu.VMEM((PAIRS, IMG_DEV, 128), F32),
        ],
        name="select",
    )(pair_table, slot_image.reshape(slots // 128, 128), slot_view.reshape(slots // 128, 128), embeddings)


def shift_of(plane, core):
    return 7 + core + 4 * (plane // 2)


def cross_kernel(
    x1_ref, x2_ref, stat_ref, out_ref,
    x1p, x1a, x1ap, x2b, statb, x1stat, cb, relay_p, relay_m, from_m, from_p, total, yr, fs, fr,
    z_send, z_recv, x_send, x_recv, y_send, y_recv, f_send, f_recv,
):
    y, x, zl, h, core = [lax.axis_index(axis) for axis in AXES]
    plane_a = h + 1 - 2 * (h % 2)
    plane_b = 3 - h
    other = 1 - core
    xp, xa, xm = (x + 1) % NX, (x + 2) % NX, (x + 3) % NX
    yp, ym = (y + 1) % NY, (y + NY - 1) % NY
    mine = (y + 2 * NY - shift_of(h, core)) % NY

    jb, ih, half = mine // 4, (mine // 2) % 2, mine % 2
    owner_y = 2 * (h + jb * (3 - 2 * h)) + core
    owner_h = h + ih * (1 - 2 * (h % 2))
    at_home = (owner_y == y) & (owner_h == h) & (half == core)
    jh, src_core = y // 2, y % 2
    src_jb = (jh // 2 + h // 2) % 2
    src_h = jh + src_jb * (3 - 2 * jh)
    src_ih = (src_h + h) % 2
    src_y = (4 * src_jb + 2 * src_ih + core + shift_of(src_h, src_core)) % NY

    barrier = pltpu.get_barrier_semaphore()
    for peer in ({"x": xp}, {"x": xm}, {"y": yp}, {"y": ym}, {"zh": plane_a}, {"zh": plane_b}, {"core": other}):
        pl.semaphore_signal(barrier, inc=1, device_id=peer, device_id_type=MESH)
    for part in range(2):

        @pl.when(jnp.logical_not(at_home & (zl == part)))
        def _():
            pl.semaphore_signal(
                barrier,
                inc=1,
                device_id={"y": src_y, "zl": part, "zh": src_h, "core": src_core},
                device_id_type=MESH,
            )

    pl.semaphore_wait(barrier, 9 - at_home.astype(jnp.int32))

    sent = []

    def send(src, dst, send_sem, recv_sem, peer):
        copy = pltpu.make_async_remote_copy(
            src_ref=src, dst_ref=dst, send_sem=send_sem, recv_sem=recv_sem, device_id=peer, device_id_type=MESH
        )
        copy.start()
        sent.append(copy)
        return copy

    z = {}
    for pair in range(PAIRS):
        for slot, (name, src, dst, peer) in enumerate(
            (
                ("p", x1_ref, x1p, {"core": other}),
                ("b", x2_ref, x2b, {"zh": plane_b}),
                ("s", stat_ref, statb, {"zh": plane_b}),
                ("a", x1_ref, x1a, {"zh": plane_a}),
            )
        ):
            z[name, pair] = send(src.at[pair], dst.at[pair], z_send.at[pair, slot], z_recv.at[pair, slot], peer)

    def forward(pair):
        z["a", pair].wait_recv()
        z["ap", pair] = send(
            x1a.at[pair], x1ap.at[pair], z_send.at[pair, 4], z_recv.at[pair, 4], {"core": other}
        )

    stats_done = set()
    xc = {}

    def block_of(pair, jb, ih):
        return 4 * pair + 2 * jb + ih

    def multiply(pair, jb, ih):
        k = block_of(pair, jb, ih)
        second = (x2b if jb else x2_ref)[pair]
        stat = (statb if jb else stat_ref)[pair]
        row = lax.broadcasted_iota(jnp.int32, (STAT, WIDTH), 0)
        for slot, (ref, half) in enumerate((((x1a if ih else x1_ref), core), ((x1ap if ih else x1p), other))):
            first = ref[pair]
            if (pair, ih, slot) not in stats_done:
                stats_done.add((pair, ih, slot))
                wide = first.astype(F32)
                plain = jnp.sum(wide, axis=0, keepdims=True)
                square = jnp.sum(wide * wide, axis=0, keepdims=True)
                x1stat[pair, ih, slot] = jnp.where(row == 0, plain, jnp.where(row == 1, square, 0.0))
            product = jnp.dot(second, first, preferred_element_type=F32)
            sums = x1stat[pair, ih, slot] + stat
            for dest in range(NX):
                cb[k, dest, half, 0:BLOCK] = product[dest * BLOCK : (dest + 1) * BLOCK]
                cb[k, dest, half, BLOCK:ROWS] = sums
        for slot, (src, dst, to) in enumerate(
            (
                (cb.at[k, xa, 0], relay_p.at[k], xp),
                (cb.at[k, xa, 1], relay_m.at[k], xm),
                (cb.at[k, xp, 1], from_m.at[k, 1], xp),
                (cb.at[k, xm, 0], from_p.at[k, 0], xm),
            )
        ):
            xc[k, slot] = send(src, dst, x_send.at[k, slot], x_recv.at[k, slot], {"x": to})

    def pass_on(pair, jb, ih):
        k = block_of(pair, jb, ih)
        xc[k, 0].wait_recv()
        cb[k, xp, 0] += relay_p[k]
        xc[k, 4] = send(cb.at[k, xp, 0], from_m.at[k, 0], x_send.at[k, 4], x_recv.at[k, 4], {"x": xp})
        xc[k, 1].wait_recv()
        cb[k, xm, 1] += relay_m[k]
        xc[k, 5] = send(cb.at[k, xm, 1], from_p.at[k, 1], x_send.at[k, 5], x_recv.at[k, 5], {"x": xm})

    def collect(pair, jb, ih):
        k = block_of(pair, jb, ih)
        for slot in (2, 3, 4, 5):
            xc[k, slot].wait_recv()
        for half in range(2):
            total[pair, 4 * jb + 2 * ih + half] = cb[k, x, half] + from_m[k, half] + from_p[k, half]

    yc = {}

    def y_send_part(pair, way, step, src, dst):
        to = ym if way else yp
        yc[pair, way, step] = send(
            src, dst, y_send.at[pair, way, step], y_recv.at[pair, way, step], {"y": to}
        )

    def y_step(pair, step):
        for way in range(2):
            ahead = (mine + (4 + step if way else 4 - step)) % NY
            rows = slice(CUT, ROWS) if way else slice(0, CUT)
            size = ROWS - CUT if way else CUT
            if step == 0:
                y_send_part(pair, way, 0, total.at[pair, ahead, rows], yr.at[pair, way, 0, 0:size])
                continue
            yc[pair, way, step - 1].wait_recv()
            if step == 1:
                total[pair, ahead, rows] += yr[pair, way, 0, 0:size]
            else:
                total[pair, ahead] += yr[pair, way, step - 1]
            y_send_part(pair, way, step, total.at[pair, ahead], yr.at[pair, way, step])

    def deliver(pair):
        for way in range(2):
            yc[pair, way, 3].wait_recv()
        done = total[pair, mine] + yr[pair, 0, 3] + yr[pair, 1, 3]
        for part in range(2):
            fs[pair, part, 0:OWN] = done[part * OWN : (part + 1) * OWN]
            fs[pair, part, OWN:PART] = done[BLOCK:ROWS]
            same = at_home & (zl == part)

            @pl.when(same)
            def _():
                fr[pair, zl] = fs[pair, part]

            @pl.when(jnp.logical_not(same))
            def _():
                final_copy(pair, part).start()

    def final_copy(pair, part):
        return pltpu.make_async_remote_copy(
            src_ref=fs.at[pair, part],
            dst_ref=fr.at[pair, zl],
            send_sem=f_send.at[pair, part],
            recv_sem=f_recv.at[pair, zl],
            device_id={"y": owner_y, "zl": part, "zh": owner_h, "core": half},
            device_id_type=MESH,
        )

    def receive(pair):
        for part in range(2):

            @pl.when(jnp.logical_not(at_home & (zl == part)))
            def _():
                pltpu.make_async_remote_copy(
                    src_ref=fs.at[pair, part],
                    dst_ref=fr.at[pair, part],
                    send_sem=f_send.at[pair, part],
                    recv_sem=f_recv.at[pair, part],
                    device_id={"y": owner_y, "zl": part, "zh": owner_h, "core": half},
                    device_id_type=MESH,
                ).wait_recv()

        out_ref[pair] = fr[pair, 0] + fr[pair, 1]

    for pair in range(PAIRS):
        z["p", pair].wait_recv()
        multiply(pair, 0, 0)
    for pair in range(PAIRS):
        pass_on(pair, 0, 0)

    z["b", 0].wait_recv()
    z["s", 0].wait_recv()
    multiply(0, 1, 0)
    forward(0)
    pass_on(0, 1, 0)
    z["ap", 0].wait_recv()
    multiply(0, 0, 1)
    multiply(0, 1, 1)
    pass_on(0, 0, 1)
    pass_on(0, 1, 1)
    collect(0, 0, 0)
    collect(1, 0, 0)
    collect(0, 1, 0)
    collect(0, 0, 1)
    collect(0, 1, 1)
    y_step(0, 0)

    z["b", 1].wait_recv()
    z["s", 1].wait_recv()
    multiply(1, 1, 0)
    y_step(0, 1)
    forward(1)
    pass_on(1, 1, 0)
    y_step(0, 2)
    z["ap", 1].wait_recv()
    multiply(1, 0, 1)
    multiply(1, 1, 1)
    y_step(0, 3)
    pass_on(1, 0, 1)
    pass_on(1, 1, 1)
    collect(1, 1, 0)
    deliver(0)
    collect(1, 0, 1)
    collect(1, 1, 1)
    for step in range(4):
        y_step(1, step)
    receive(0)
    deliver(1)
    receive(1)

    for copy in sent:
        copy.wait_send()
    for pair in range(PAIRS):
        for part in range(2):

            @pl.when(jnp.logical_not(at_home & (zl == part)))
            def _():
                final_copy(pair, part).wait_send()


def cross(x1, x2, stat):
    blocks = 4 * PAIRS
    dma = pltpu.SemaphoreType.DMA
    vmem = pl.BlockSpec(memory_space=pltpu.VMEM)
    return pl.pallas_call(
        cross_kernel,
        out_shape=jax.ShapeDtypeStruct((PAIRS, PART, WIDTH), F32),
        in_specs=[vmem, vmem, vmem],
        out_specs=vmem,
        scratch_shapes=[
            pltpu.VMEM((PAIRS, IMG_DEV, WIDTH), BF16),
            pltpu.VMEM((PAIRS, IMG_DEV, WIDTH), BF16),
            pltpu.VMEM((PAIRS, IMG_DEV, WIDTH), BF16),
            pltpu.VMEM((PAIRS, WIDTH, IMG_DEV), BF16),
            pltpu.VMEM((PAIRS, STAT, WIDTH), F32),
            pltpu.VMEM((PAIRS, 2, 2, STAT, WIDTH), F32),
            pltpu.VMEM((blocks, NX, 2, ROWS, WIDTH), F32),
            pltpu.VMEM((blocks, ROWS, WIDTH), F32),
            pltpu.VMEM((blocks, ROWS, WIDTH), F32),
            pltpu.VMEM((blocks, 2, ROWS, WIDTH), F32),
            pltpu.VMEM((blocks, 2, ROWS, WIDTH), F32),
            pltpu.VMEM((PAIRS, NY, ROWS, WIDTH), F32),
            pltpu.VMEM((PAIRS, 2, 4, ROWS, WIDTH), F32),
            pltpu.VMEM((PAIRS, 2, PART, WIDTH), F32),
            pltpu.VMEM((PAIRS, 2, PART, WIDTH), F32),
            dma((PAIRS, 5)),
            dma((PAIRS, 5)),
            dma((blocks, 6)),
            dma((blocks, 6)),
            dma((PAIRS, 2, 4)),
            dma((PAIRS, 2, 4)),
            dma((PAIRS, 2)),
            dma((PAIRS, 2)),
        ],
        compiler_params=pltpu.CompilerParams(collective_id=0, has_side_effects=True),
        name="cross",
    )(x1, x2, stat)


def local(embeddings, slot_image, slot_view, pair_table):
    summed = cross(*select(pair_table, slot_image, slot_view, embeddings))
    offset = lax.axis_index("x") * BLOCK + lax.axis_index("zl") * OWN
    products = summed[:, :OWN]
    count = summed[:, OWN + 4, 0][:, None]
    mean_first = summed[:, OWN] / count
    square_first = summed[:, OWN + 1] / count
    mean_second = lax.dynamic_slice_in_dim(summed[:, OWN + 2], offset, OWN, 1) / count
    square_second = lax.dynamic_slice_in_dim(summed[:, OWN + 3], offset, OWN, 1) / count
    spread_first = jnp.sqrt(square_first - mean_first * mean_first + EPS)
    spread_second = jnp.sqrt(square_second - mean_second * mean_second + EPS)
    block = (products / count[:, :, None] - mean_second[:, :, None] * mean_first[:, None, :]) / (
        spread_second[:, :, None] * spread_first[:, None, :]
    )
    return jnp.swapaxes(block, 1, 2)


def solution(mesh):
    split = Mesh(mesh.devices.reshape(NY, NX, 2, 4, 2), AXES)
    placed = (P(DP, FEAT), P(DP), P(DP), P())
    return jax.shard_map(local, mesh=split, in_specs=placed, out_specs=P(None, FEAT, DP), check_vma=False)
```

```python
import jax
import jax.numpy as jnp
from jax import lax
from jax.experimental import pallas as pl
from jax.experimental.pallas import tpu as pltpu
from jax.sharding import Mesh
from jax.sharding import PartitionSpec as P

WIN = 2048
IMG_DEV = 512
PAIRS = 2
WIDTH = 256
OWN = 32
NX, NY = 4, 8
BLOCK = 64
STAT = 8
ROWS = BLOCK + STAT
PART = OWN + STAT
CUT = 40
SLOTS = 1024
STEPS = 5
TILE = SLOTS // 128
VIEW_STRIDE = 16
AXES = ("y", "x", "zl", "zh", "core")
FEAT = ("zh", "core")
DP = ("y", "x", "zl")
EPS = 1e-05
F32 = jnp.float32
BF16 = jnp.bfloat16
MESH = pl.DeviceIdType.MESH


def shift_of(plane, core):
    return 7 + core + 4 * (plane // 2)


def cross_kernel(
    pair_ref, image_ref, view_ref, emb_ref, out_ref,
    emb, acc, found, x1_ref, x2_ref, stat_ref,
    x1p, x1a, x1ap, x2b, statb, x1stat, cb, relay_p, relay_m, from_m, from_p, total, yr, fs, fr,
    emb_sem, z_send, z_recv, x_send, x_recv, y_send, y_recv, f_send, f_recv,
):
    y, x, zl, h, core = [lax.axis_index(axis) for axis in AXES]
    plane_a = h + 1 - 2 * (h % 2)
    plane_b = 3 - h
    other = 1 - core
    xp, xa, xm = (x + 1) % NX, (x + 2) % NX, (x + 3) % NX
    yp, ym = (y + 1) % NY, (y + NY - 1) % NY
    mine = (y + 2 * NY - shift_of(h, core)) % NY

    jb, ih, half = mine // 4, (mine // 2) % 2, mine % 2
    owner_y = 2 * (h + jb * (3 - 2 * h)) + core
    owner_h = h + ih * (1 - 2 * (h % 2))
    at_home = (owner_y == y) & (owner_h == h) & (half == core)
    jh, src_core = y // 2, y % 2
    src_jb = (jh // 2 + h // 2) % 2
    src_h = jh + src_jb * (3 - 2 * jh)
    src_ih = (src_h + h) % 2
    src_y = (4 * src_jb + 2 * src_ih + core + shift_of(src_h, src_core)) % NY

    loads = []
    for step in range(STEPS):
        rows = slice(step * SLOTS, (step + 1) * SLOTS)
        loads.append(pltpu.make_async_copy(emb_ref.at[rows], emb.at[rows], emb_sem.at[step]))
        loads[-1].start()

    barrier = pltpu.get_barrier_semaphore()
    for peer in ({"x": xp}, {"x": xm}, {"y": yp}, {"y": ym}, {"zh": plane_a}, {"zh": plane_b}, {"core": other}):
        pl.semaphore_signal(barrier, inc=1, device_id=peer, device_id_type=MESH)
    for part in range(2):

        @pl.when(jnp.logical_not(at_home & (zl == part)))
        def _():
            pl.semaphore_signal(
                barrier,
                inc=1,
                device_id={"y": src_y, "zl": part, "zh": src_h, "core": src_core},
                device_id_type=MESH,
            )

    sent = []

    def send(src, dst, send_sem, recv_sem, peer):
        copy = pltpu.make_async_remote_copy(
            src_ref=src, dst_ref=dst, send_sem=send_sem, recv_sem=recv_sem, device_id=peer, device_id_type=MESH
        )
        copy.start()
        sent.append(copy)
        return copy

    z = {}

    def offer(pair, name):
        slot, src, dst, peer = {
            "p": (0, x1_ref, x1p, {"core": other}),
            "b": (1, x2_ref, x2b, {"zh": plane_b}),
            "s": (2, stat_ref, statb, {"zh": plane_b}),
            "a": (3, x1_ref, x1a, {"zh": plane_a}),
        }[name]
        z[name, pair] = send(src.at[pair], dst.at[pair], z_send.at[pair, slot], z_recv.at[pair, slot], peer)

    def arrive(pair, *names):
        for name in names:
            z[name, pair].wait_recv()

    base = (y * NX * 2 + x * 2 + zl) * IMG_DEV
    wanted = (lax.broadcasted_iota(jnp.int32, (IMG_DEV, 128), 0) + base) * VIEW_STRIDE

    def pick(pair, side):
        target = wanted + pair_ref[pair, side]
        acc[...] = jnp.zeros_like(acc)
        if side:
            found[pair] = jnp.zeros_like(found[pair])

        def step(index, carry):
            key = image_ref[pl.ds(pl.multiple_of(index * TILE, TILE), TILE), :] * VIEW_STRIDE
            key += view_ref[pl.ds(pl.multiple_of(index * TILE, TILE), TILE), :]
            hits = [jnp.where(key[row : row + 1, :] == target, 1.0, 0.0) for row in range(TILE)]
            chosen = jnp.concatenate([hit.astype(BF16) for hit in hits], axis=1)
            rows = emb[pl.ds(pl.multiple_of(index * SLOTS, SLOTS), SLOTS), :]
            acc[...] += jnp.dot(chosen, rows, preferred_element_type=F32)
            if side:
                found[pair] += sum(hits[1:], hits[0])
            return carry

        lax.fori_loop(0, STEPS, step, 0)

    def pick_second(pair):
        pick(pair, 1)
        row = lax.broadcasted_iota(jnp.int32, (STAT, WIDTH), 0)
        second = acc[...]
        x2_ref[pair] = second.T.astype(BF16)
        plain = jnp.sum(second, axis=0, keepdims=True)
        square = jnp.sum(second * second, axis=0, keepdims=True)
        count = jnp.sum(found[pair])
        stat_ref[pair] = jnp.where(
            row == 2, plain, jnp.where(row == 3, square, jnp.where(row == 4, count, 0.0))
        )

    def pick_first(pair):
        pick(pair, 0)
        present = jnp.sum(found[pair], axis=1, keepdims=True)
        x1_ref[pair] = jnp.where(present > 0.5, acc[...], 0.0).astype(BF16)

    def forward(pair):
        arrive(pair, "a")
        z["ap", pair] = send(
            x1a.at[pair], x1ap.at[pair], z_send.at[pair, 4], z_recv.at[pair, 4], {"core": other}
        )

    stats_done = set()
    xc = {}

    def block_of(pair, jb, ih):
        return 4 * pair + 2 * jb + ih

    def multiply(pair, jb, ih):
        k = block_of(pair, jb, ih)
        second = (x2b if jb else x2_ref)[pair]
        stat = (statb if jb else stat_ref)[pair]
        row = lax.broadcasted_iota(jnp.int32, (STAT, WIDTH), 0)
        for slot, (ref, half) in enumerate((((x1a if ih else x1_ref), core), ((x1ap if ih else x1p), other))):
            first = ref[pair]
            if (pair, ih, slot) not in stats_done:
                stats_done.add((pair, ih, slot))
                wide = first.astype(F32)
                plain = jnp.sum(wide, axis=0, keepdims=True)
                square = jnp.sum(wide * wide, axis=0, keepdims=True)
                x1stat[pair, ih, slot] = jnp.where(row == 0, plain, jnp.where(row == 1, square, 0.0))
            product = jnp.dot(second, first, preferred_element_type=F32)
            sums = x1stat[pair, ih, slot] + stat
            for dest in range(NX):
                cb[k, dest, half, 0:BLOCK] = product[dest * BLOCK : (dest + 1) * BLOCK]
                cb[k, dest, half, BLOCK:ROWS] = sums
        for slot, (src, dst, to) in enumerate(
            (
                (cb.at[k, xa, 0], relay_p.at[k], xp),
                (cb.at[k, xa, 1], relay_m.at[k], xm),
                (cb.at[k, xp, 1], from_m.at[k, 1], xp),
                (cb.at[k, xm, 0], from_p.at[k, 0], xm),
            )
        ):
            xc[k, slot] = send(src, dst, x_send.at[k, slot], x_recv.at[k, slot], {"x": to})

    def pass_on(pair, jb, ih):
        k = block_of(pair, jb, ih)
        xc[k, 0].wait_recv()
        cb[k, xp, 0] += relay_p[k]
        xc[k, 4] = send(cb.at[k, xp, 0], from_m.at[k, 0], x_send.at[k, 4], x_recv.at[k, 4], {"x": xp})
        xc[k, 1].wait_recv()
        cb[k, xm, 1] += relay_m[k]
        xc[k, 5] = send(cb.at[k, xm, 1], from_p.at[k, 1], x_send.at[k, 5], x_recv.at[k, 5], {"x": xm})

    def collect(pair, jb, ih):
        k = block_of(pair, jb, ih)
        for slot in (2, 3, 4, 5):
            xc[k, slot].wait_recv()
        for half in range(2):
            total[pair, 4 * jb + 2 * ih + half] = cb[k, x, half] + from_m[k, half] + from_p[k, half]

    yc = {}

    def y_send_part(pair, way, step, src, dst):
        to = ym if way else yp
        yc[pair, way, step] = send(
            src, dst, y_send.at[pair, way, step], y_recv.at[pair, way, step], {"y": to}
        )

    def y_step(pair, step):
        for way in range(2):
            ahead = (mine + (4 + step if way else 4 - step)) % NY
            rows = slice(CUT, ROWS) if way else slice(0, CUT)
            size = ROWS - CUT if way else CUT
            if step == 0:
                y_send_part(pair, way, 0, total.at[pair, ahead, rows], yr.at[pair, way, 0, 0:size])
                continue
            yc[pair, way, step - 1].wait_recv()
            if step == 1:
                total[pair, ahead, rows] += yr[pair, way, 0, 0:size]
            else:
                total[pair, ahead] += yr[pair, way, step - 1]
            y_send_part(pair, way, step, total.at[pair, ahead], yr.at[pair, way, step])

    def deliver(pair):
        for way in range(2):
            yc[pair, way, 3].wait_recv()
        done = total[pair, mine] + yr[pair, 0, 3] + yr[pair, 1, 3]
        for part in range(2):
            fs[pair, part, 0:OWN] = done[part * OWN : (part + 1) * OWN]
            fs[pair, part, OWN:PART] = done[BLOCK:ROWS]
            same = at_home & (zl == part)

            @pl.when(same)
            def _():
                fr[pair, zl] = fs[pair, part]

            @pl.when(jnp.logical_not(same))
            def _():
                final_copy(pair, part).start()

    def final_copy(pair, part):
        return pltpu.make_async_remote_copy(
            src_ref=fs.at[pair, part],
            dst_ref=fr.at[pair, zl],
            send_sem=f_send.at[pair, part],
            recv_sem=f_recv.at[pair, zl],
            device_id={"y": owner_y, "zl": part, "zh": owner_h, "core": half},
            device_id_type=MESH,
        )

    def receive(pair):
        for part in range(2):

            @pl.when(jnp.logical_not(at_home & (zl == part)))
            def _():
                pltpu.make_async_remote_copy(
                    src_ref=fs.at[pair, part],
                    dst_ref=fr.at[pair, part],
                    send_sem=f_send.at[pair, part],
                    recv_sem=f_recv.at[pair, part],
                    device_id={"y": owner_y, "zl": part, "zh": owner_h, "core": half},
                    device_id_type=MESH,
                ).wait_recv()

        both = fr[pair, 0] + fr[pair, 1]
        count = both[OWN + 4 : OWN + 5, 0:1]
        lane = lax.broadcasted_iota(jnp.int32, (OWN, WIDTH), 1)
        row = lax.broadcasted_iota(jnp.int32, (OWN, WIDTH), 0)
        own = lane == row + (x * BLOCK + zl * OWN)

        def column(line):
            return jnp.sum(jnp.where(own, line, 0.0), axis=1, keepdims=True)

        mean_first = both[OWN : OWN + 1] / count
        square_first = both[OWN + 1 : OWN + 2] / count
        mean_second = column(both[OWN + 2 : OWN + 3]) / count
        square_second = column(both[OWN + 3 : OWN + 4]) / count
        spread_first = jnp.sqrt(square_first - mean_first * mean_first + EPS)
        spread_second = jnp.sqrt(square_second - mean_second * mean_second + EPS)
        out_ref[pair] = (both[0:OWN] / count - mean_second * mean_first) / (spread_second * spread_first)

    for load in loads:
        load.wait()
    pick_second(0)
    pl.semaphore_wait(barrier, 9 - at_home.astype(jnp.int32))
    offer(0, "b")
    offer(0, "s")
    pick_first(0)
    offer(0, "a")
    offer(0, "p")
    pick_second(1)
    offer(1, "b")
    offer(1, "s")
    arrive(0, "p")
    multiply(0, 0, 0)
    pick_first(1)
    offer(1, "a")
    offer(1, "p")
    pass_on(0, 0, 0)
    arrive(1, "p")
    multiply(1, 0, 0)
    arrive(0, "b", "s")
    multiply(0, 1, 0)
    pass_on(1, 0, 0)
    forward(0)
    pass_on(0, 1, 0)
    arrive(0, "ap")
    multiply(0, 0, 1)
    multiply(0, 1, 1)
    pass_on(0, 0, 1)
    pass_on(0, 1, 1)
    collect(0, 0, 0)
    collect(1, 0, 0)
    collect(0, 1, 0)
    arrive(1, "b", "s")
    multiply(1, 1, 0)
    forward(1)
    collect(0, 0, 1)
    arrive(1, "ap")
    multiply(1, 0, 1)
    multiply(1, 1, 1)
    pass_on(1, 1, 0)
    collect(0, 1, 1)
    y_step(0, 0)
    pass_on(1, 0, 1)
    y_step(0, 1)
    pass_on(1, 1, 1)
    y_step(0, 2)
    collect(1, 1, 0)
    y_step(0, 3)
    collect(1, 0, 1)
    deliver(0)
    collect(1, 1, 1)
    y_step(1, 0)
    y_step(1, 1)
    receive(0)
    y_step(1, 2)
    y_step(1, 3)
    deliver(1)
    receive(1)

    for copy in sent:
        copy.wait_send()
    for pair in range(PAIRS):
        for part in range(2):

            @pl.when(jnp.logical_not(at_home & (zl == part)))
            def _():
                final_copy(pair, part).wait_send()


def cross(pair_table, image, view, embeddings):
    blocks = 4 * PAIRS
    dma = pltpu.SemaphoreType.DMA
    vmem = pl.BlockSpec(memory_space=pltpu.VMEM)
    return pl.pallas_call(
        cross_kernel,
        out_shape=jax.ShapeDtypeStruct((PAIRS, OWN, WIDTH), F32),
        in_specs=[pl.BlockSpec(memory_space=pltpu.SMEM), vmem, vmem, pl.BlockSpec(memory_space=pl.ANY)],
        out_specs=vmem,
        scratch_shapes=[
            pltpu.VMEM((STEPS * SLOTS, WIDTH), BF16),
            pltpu.VMEM((IMG_DEV, WIDTH), F32),
            pltpu.VMEM((PAIRS, IMG_DEV, 128), F32),
            pltpu.VMEM((PAIRS, IMG_DEV, WIDTH), BF16),
            pltpu.VMEM((PAIRS, WIDTH, IMG_DEV), BF16),
            pltpu.VMEM((PAIRS, STAT, WIDTH), F32),
            pltpu.VMEM((PAIRS, IMG_DEV, WIDTH), BF16),
            pltpu.VMEM((PAIRS, IMG_DEV, WIDTH), BF16),
            pltpu.VMEM((PAIRS, IMG_DEV, WIDTH), BF16),
            pltpu.VMEM((PAIRS, WIDTH, IMG_DEV), BF16),
            pltpu.VMEM((PAIRS, STAT, WIDTH), F32),
            pltpu.VMEM((PAIRS, 2, 2, STAT, WIDTH), F32),
            pltpu.VMEM((blocks, NX, 2, ROWS, WIDTH), F32),
            pltpu.VMEM((blocks, ROWS, WIDTH), F32),
            pltpu.VMEM((blocks, ROWS, WIDTH), F32),
            pltpu.VMEM((blocks, 2, ROWS, WIDTH), F32),
            pltpu.VMEM((blocks, 2, ROWS, WIDTH), F32),
            pltpu.VMEM((PAIRS, NY, ROWS, WIDTH), F32),
            pltpu.VMEM((PAIRS, 2, 4, ROWS, WIDTH), F32),
            pltpu.VMEM((PAIRS, 2, PART, WIDTH), F32),
            pltpu.VMEM((PAIRS, 2, PART, WIDTH), F32),
            dma((STEPS,)),
            dma((PAIRS, 5)),
            dma((PAIRS, 5)),
            dma((blocks, 6)),
            dma((blocks, 6)),
            dma((PAIRS, 2, 4)),
            dma((PAIRS, 2, 4)),
            dma((PAIRS, 2)),
            dma((PAIRS, 2)),
        ],
        compiler_params=pltpu.CompilerParams(collective_id=0, has_side_effects=True),
        name="cross",
    )(pair_table, image, view, embeddings)


def local(embeddings, slot_image, slot_view, pair_table):
    shape = (STEPS * TILE, 128)
    block = cross(pair_table, slot_image.reshape(shape), slot_view.reshape(shape), embeddings)
    return jnp.swapaxes(block, 1, 2)


def solution(mesh):
    split = Mesh(mesh.devices.reshape(NY, NX, 2, 4, 2), AXES)
    placed = (P(DP, FEAT), P(DP), P(DP), P())
    return jax.shard_map(local, mesh=split, in_specs=placed, out_specs=P(None, FEAT, DP), check_vma=False)
```

```python
import jax
import jax.numpy as jnp
from jax import lax
from jax.experimental import pallas as pl
from jax.experimental.pallas import tpu as pltpu
from jax.sharding import Mesh
from jax.sharding import PartitionSpec as P

WIN = 2048
IMG_DEV = 512
PAIRS = 2
WIDTH = 256
OWN = 32
NX, NY = 4, 8
BLOCK = 64
STAT = 8
LEAD = 40
REST = BLOCK - LEAD
ROWS = LEAD + STAT
PART = OWN + STAT
CUT = 24
REST_CUT = 16
GROUPS = (
    ((0, 0, 0), (1, 0, 0)),
    ((0, 1, 0), (0, 0, 1), (0, 1, 1)),
    ((1, 1, 0), (1, 0, 1), (1, 1, 1)),
)
SLOTS = 1024
STEPS = 5
TILE = SLOTS // 128
VIEW_STRIDE = 16
AXES = ("y", "x", "zl", "zh", "core")
FEAT = ("zh", "core")
DP = ("y", "x", "zl")
EPS = 1e-05
F32 = jnp.float32
BF16 = jnp.bfloat16
MESH = pl.DeviceIdType.MESH


def shift_of(plane, core):
    return 7 + core + 4 * (plane // 2)


def cross_kernel(
    pair_ref, image_ref, view_ref, emb_ref, out_ref,
    emb, acc, found, counts, x1_ref, x2_ref, stat_ref,
    x1p, x1a, x1ap, x2b, statb, x1stat, cb, relay_p, relay_m, from_m, from_p, total, yr, fs, fr,
    w0, w1, w2, v0, v1, v2, rest, rest_in,
    emb_sem, z_send, z_recv, x_send, x_recv, y_send, y_recv, f_send, f_recv, w_send, w_recv, r_send, r_recv,
):
    y, x, zl, h, core = [lax.axis_index(axis) for axis in AXES]
    plane_a = h + 1 - 2 * (h % 2)
    plane_b = 3 - h
    other = 1 - core
    xp, xa, xm = (x + 1) % NX, (x + 2) % NX, (x + 3) % NX
    yp, ym = (y + 1) % NY, (y + NY - 1) % NY
    mine = (y + 2 * NY - shift_of(h, core)) % NY

    jb, ih, half = mine // 4, (mine // 2) % 2, mine % 2
    owner_y = 2 * (h + jb * (3 - 2 * h)) + core
    owner_h = h + ih * (1 - 2 * (h % 2))
    at_home = (owner_y == y) & (owner_h == h) & (half == core)
    jh, src_core = y // 2, y % 2
    src_jb = (jh // 2 + h // 2) % 2
    src_h = jh + src_jb * (3 - 2 * jh)
    src_ih = (src_h + h) % 2
    src_y = (4 * src_jb + 2 * src_ih + core + shift_of(src_h, src_core)) % NY
    rest_y = 2 * x + core
    rest_home = (rest_y == y) & (src_h == h) & (zl == 1)

    loads = []
    for step in range(STEPS):
        rows = slice(step * SLOTS, (step + 1) * SLOTS)
        loads.append(pltpu.make_async_copy(emb_ref.at[rows], emb.at[rows], emb_sem.at[step]))
        loads[-1].start()

    barrier = pltpu.get_barrier_semaphore()
    for peer in ({"x": xp}, {"x": xm}, {"y": yp}, {"y": ym}, {"zh": plane_a}, {"zh": plane_b}, {"core": other}):
        pl.semaphore_signal(barrier, inc=1, device_id=peer, device_id_type=MESH)
    for part in range(2):

        @pl.when(jnp.logical_not(at_home & (zl == part)))
        def _():
            pl.semaphore_signal(
                barrier,
                inc=1,
                device_id={"y": src_y, "zl": part, "zh": src_h, "core": src_core},
                device_id_type=MESH,
            )

    for from_x in range(NX):
        for part in range(2):

            @pl.when((zl == 1) & jnp.logical_not(rest_home & (x == from_x) & (zl == part)))
            def _():
                pl.semaphore_signal(
                    barrier,
                    inc=1,
                    device_id={"y": rest_y, "x": from_x, "zl": part, "zh": src_h, "core": src_core},
                    device_id_type=MESH,
                )

    sent = []

    def send(src, dst, send_sem, recv_sem, peer):
        copy = pltpu.make_async_remote_copy(
            src_ref=src, dst_ref=dst, send_sem=send_sem, recv_sem=recv_sem, device_id=peer, device_id_type=MESH
        )
        copy.start()
        sent.append(copy)
        return copy

    z = {}

    def offer(pair, name):
        slot, src, dst, peer = {
            "p": (0, x1_ref, x1p, {"core": other}),
            "b": (1, x2_ref, x2b, {"zh": plane_b}),
            "s": (2, stat_ref, statb, {"zh": plane_b}),
            "a": (3, x1_ref, x1a, {"zh": plane_a}),
        }[name]
        z[name, pair] = send(src.at[pair], dst.at[pair], z_send.at[pair, slot], z_recv.at[pair, slot], peer)

    def arrive(pair, *names):
        for name in names:
            z[name, pair].wait_recv()

    base = (y * NX * 2 + x * 2 + zl) * IMG_DEV
    wanted = (lax.broadcasted_iota(jnp.int32, (IMG_DEV, 128), 0) + base) * VIEW_STRIDE

    def pick(pair, side):
        target = wanted + pair_ref[pair, side]
        second = wanted + pair_ref[pair, 1]
        acc[...] = jnp.zeros_like(acc)
        if side == 0:
            found[...] = jnp.zeros_like(found)

        def step(index, carry):
            key = image_ref[pl.ds(pl.multiple_of(index * TILE, TILE), TILE), :] * VIEW_STRIDE
            key += view_ref[pl.ds(pl.multiple_of(index * TILE, TILE), TILE), :]
            keys = [key[row : row + 1, :] for row in range(TILE)]
            chosen = jnp.concatenate([jnp.where(one == target, 1.0, 0.0).astype(BF16) for one in keys], axis=1)
            rows = emb[pl.ds(pl.multiple_of(index * SLOTS, SLOTS), SLOTS), :]
            acc[...] += jnp.dot(chosen, rows, preferred_element_type=F32)
            if side == 0:
                hits = [jnp.where(one == second, 1.0, 0.0) for one in keys]
                found[...] += sum(hits[1:], hits[0])
            return carry

        lax.fori_loop(0, STEPS, step, 0)

    def pick_first(pair):
        pick(pair, 0)
        present = jnp.sum(found[...], axis=1, keepdims=True)
        x1_ref[pair] = jnp.where(present > 0.5, acc[...], 0.0).astype(BF16)
        counts[pair] = jnp.broadcast_to(jnp.sum(present, axis=0, keepdims=True), (1, WIDTH))

    def pick_second(pair):
        pick(pair, 1)
        row = lax.broadcasted_iota(jnp.int32, (STAT, WIDTH), 0)
        rows = acc[...]
        x2_ref[pair] = rows.T.astype(BF16)
        plain = jnp.sum(rows, axis=0, keepdims=True)
        square = jnp.sum(rows * rows, axis=0, keepdims=True)
        stat_ref[pair] = jnp.where(
            row == 2, plain, jnp.where(row == 3, square, jnp.where(row == 4, counts[pair], 0.0))
        )

    def forward(pair):
        arrive(pair, "a")
        z["ap", pair] = send(
            x1a.at[pair], x1ap.at[pair], z_send.at[pair, 4], z_recv.at[pair, 4], {"core": other}
        )

    stats_done = set()
    xc = {}

    def block_of(pair, jb, ih):
        return 4 * pair + 2 * jb + ih

    def multiply(pair, jb, ih):
        k = block_of(pair, jb, ih)
        group, place = next(
            (g, blocks.index((pair, jb, ih))) for g, blocks in enumerate(GROUPS) if (pair, jb, ih) in blocks
        )
        second = (x2b if jb else x2_ref)[pair]
        stat = (statb if jb else stat_ref)[pair]
        row = lax.broadcasted_iota(jnp.int32, (STAT, WIDTH), 0)
        for slot, (ref, half) in enumerate((((x1a if ih else x1_ref), core), ((x1ap if ih else x1p), other))):
            first = ref[pair]
            if (pair, ih, slot) not in stats_done:
                stats_done.add((pair, ih, slot))
                wide = first.astype(F32)
                plain = jnp.sum(wide, axis=0, keepdims=True)
                square = jnp.sum(wide * wide, axis=0, keepdims=True)
                x1stat[pair, ih, slot] = jnp.where(row == 0, plain, jnp.where(row == 1, square, 0.0))
            product = jnp.dot(second, first, preferred_element_type=F32)
            sums = x1stat[pair, ih, slot] + stat
            for dest in range(NX):
                cb[k, dest, half, 0:LEAD] = product[dest * BLOCK : dest * BLOCK + LEAD]
                cb[k, dest, half, LEAD:ROWS] = sums
                w[group][2 * dest + half, place] = product[dest * BLOCK + LEAD : (dest + 1) * BLOCK]
        for slot, (src, dst, to) in enumerate(
            (
                (cb.at[k, xa, 0], relay_p.at[k], xp),
                (cb.at[k, xa, 1], relay_m.at[k], xm),
                (cb.at[k, xp, 1], from_m.at[k, 1], xp),
                (cb.at[k, xm, 0], from_p.at[k, 0], xm),
            )
        ):
            xc[k, slot] = send(src, dst, x_send.at[k, slot], x_recv.at[k, slot], {"x": to})

    def pass_on(pair, jb, ih):
        k = block_of(pair, jb, ih)
        xc[k, 0].wait_recv()
        cb[k, xp, 0] += relay_p[k]
        xc[k, 4] = send(cb.at[k, xp, 0], from_m.at[k, 0], x_send.at[k, 4], x_recv.at[k, 4], {"x": xp})
        xc[k, 1].wait_recv()
        cb[k, xm, 1] += relay_m[k]
        xc[k, 5] = send(cb.at[k, xm, 1], from_p.at[k, 1], x_send.at[k, 5], x_recv.at[k, 5], {"x": xm})

    def collect(pair, jb, ih):
        k = block_of(pair, jb, ih)
        for slot in (2, 3, 4, 5):
            xc[k, slot].wait_recv()
        for half in range(2):
            total[pair, 4 * jb + 2 * ih + half] = cb[k, x, half] + from_m[k, half] + from_p[k, half]

    yc = {}

    def y_send_part(pair, way, step, src, dst):
        to = ym if way else yp
        yc[pair, way, step] = send(
            src, dst, y_send.at[pair, way, step], y_recv.at[pair, way, step], {"y": to}
        )

    def y_step(pair, step):
        for way in range(2):
            ahead = (mine + (4 + step if way else 4 - step)) % NY
            rows = slice(CUT, ROWS) if way else slice(0, CUT)
            size = ROWS - CUT if way else CUT
            if step == 0:
                y_send_part(pair, way, 0, total.at[pair, ahead, rows], yr.at[pair, way, 0, 0:size])
                continue
            yc[pair, way, step - 1].wait_recv()
            if step == 1:
                total[pair, ahead, rows] += yr[pair, way, 0, 0:size]
            else:
                total[pair, ahead] += yr[pair, way, step - 1]
            y_send_part(pair, way, step, total.at[pair, ahead], yr.at[pair, way, step])

    w, v = (w0, w1, w2), (v0, v1, v2)
    wc = {}

    def w_step(group, step):
        for way in range(2):
            ahead = (y + (4 + step if way else 4 - step)) % NY
            rows = slice(REST_CUT, REST) if way else slice(0, REST_CUT)
            size = REST - REST_CUT if way else REST_CUT
            sems = (w_send.at[group, way, step], w_recv.at[group, way, step], {"y": ym if way else yp})
            if step == 0:
                wc[group, way, 0] = send(
                    w[group].at[ahead, :, rows], v[group].at[way, 0, :, 0:size], *sems
                )
                continue
            wc[group, way, step - 1].wait_recv()
            if step == 1:
                w[group][ahead, :, rows] += v[group][way, 0, :, 0:size]
            else:
                w[group][ahead] += v[group][way, step - 1]
            wc[group, way, step] = send(w[group].at[ahead], v[group].at[way, step], *sems)

    def rest_copy(pair, jb, ih):
        k = block_of(pair, jb, ih)
        return pltpu.make_async_remote_copy(
            src_ref=rest.at[k],
            dst_ref=rest_in.at[pair, x, zl],
            send_sem=r_send.at[k],
            recv_sem=r_recv.at[pair, x, zl],
            device_id={
                "y": 2 * (plane_b if jb else h) + core,
                "x": y // 2,
                "zl": 1,
                "zh": plane_a if ih else h,
                "core": y % 2,
            },
            device_id_type=MESH,
        )

    def w_deliver(group):
        for way in range(2):
            wc[group, way, 3].wait_recv()
        for place, (pair, jb, ih) in enumerate(GROUPS[group]):
            k = block_of(pair, jb, ih)
            rest[k] = w[group][y, place] + v[group][0, 3, place] + v[group][1, 3, place]
            if ih:
                rest_copy(pair, jb, ih).start()
                continue
            same = rest_home & (src_jb == jb)

            @pl.when(same)
            def _():
                rest_in[pair, x, zl] = rest[k]

            @pl.when(jnp.logical_not(same))
            def _():
                rest_copy(pair, jb, ih).start()

    def rest_receive(pair):
        @pl.when(zl == 1)
        def _():
            for from_x in range(NX):
                for part in range(2):

                    @pl.when(jnp.logical_not(rest_home & (x == from_x) & (zl == part)))
                    def _():
                        pltpu.make_async_remote_copy(
                            src_ref=rest.at[0],
                            dst_ref=rest_in.at[pair, from_x, part],
                            send_sem=r_send.at[0],
                            recv_sem=r_recv.at[pair, from_x, part],
                            device_id={"x": xp},
                            device_id_type=MESH,
                        ).wait_recv()

            lead = OWN - REST
            summed = rest_in[pair, 0, 0]
            for slot in range(1, 2 * NX):
                summed += rest_in[pair, slot // 2, slot % 2]
            fr[pair, 0, lead:OWN] += summed

    def deliver(pair):
        for way in range(2):
            yc[pair, way, 3].wait_recv()
        done = total[pair, mine] + yr[pair, 0, 3] + yr[pair, 1, 3]
        for part in range(2):
            if part:
                fs[pair, 1, 0 : LEAD - OWN] = done[OWN:LEAD]
                fs[pair, 1, LEAD - OWN : OWN] = jnp.zeros((REST, WIDTH), F32)
            else:
                fs[pair, 0, 0:OWN] = done[0:OWN]
            fs[pair, part, OWN:PART] = done[LEAD:ROWS]
            same = at_home & (zl == part)

            @pl.when(same)
            def _():
                fr[pair, zl] = fs[pair, part]

            @pl.when(jnp.logical_not(same))
            def _():
                final_copy(pair, part).start()

    def final_copy(pair, part):
        return pltpu.make_async_remote_copy(
            src_ref=fs.at[pair, part],
            dst_ref=fr.at[pair, zl],
            send_sem=f_send.at[pair, part],
            recv_sem=f_recv.at[pair, zl],
            device_id={"y": owner_y, "zl": part, "zh": owner_h, "core": half},
            device_id_type=MESH,
        )

    def receive(pair):
        for part in range(2):

            @pl.when(jnp.logical_not(at_home & (zl == part)))
            def _():
                pltpu.make_async_remote_copy(
                    src_ref=fs.at[pair, part],
                    dst_ref=fr.at[pair, part],
                    send_sem=f_send.at[pair, part],
                    recv_sem=f_recv.at[pair, part],
                    device_id={"y": owner_y, "zl": part, "zh": owner_h, "core": half},
                    device_id_type=MESH,
                ).wait_recv()

        rest_receive(pair)
        both = fr[pair, 0] + fr[pair, 1]
        count = both[OWN + 4 : OWN + 5, 0:1]
        lane = lax.broadcasted_iota(jnp.int32, (OWN, WIDTH), 1)
        row = lax.broadcasted_iota(jnp.int32, (OWN, WIDTH), 0)
        own = lane == row + (x * BLOCK + zl * OWN)

        def column(line):
            return jnp.sum(jnp.where(own, line, 0.0), axis=1, keepdims=True)

        mean_first = both[OWN : OWN + 1] / count
        square_first = both[OWN + 1 : OWN + 2] / count
        mean_second = column(both[OWN + 2 : OWN + 3]) / count
        square_second = column(both[OWN + 3 : OWN + 4]) / count
        spread_first = jnp.sqrt(square_first - mean_first * mean_first + EPS)
        spread_second = jnp.sqrt(square_second - mean_second * mean_second + EPS)
        out_ref[pair] = (both[0:OWN] / count - mean_second * mean_first) / (spread_second * spread_first)

    for load in loads:
        load.wait()
    pick_first(0)
    pl.semaphore_wait(barrier, 13 - at_home.astype(jnp.int32) - rest_home.astype(jnp.int32))
    offer(0, "a")
    offer(0, "p")
    pick_second(0)
    offer(0, "b")
    offer(0, "s")
    arrive(0, "p")
    multiply(0, 0, 0)
    pick_first(1)
    offer(1, "a")
    offer(1, "p")
    pass_on(0, 0, 0)
    pick_second(1)
    offer(1, "b")
    offer(1, "s")
    arrive(1, "p")
    multiply(1, 0, 0)
    w_step(0, 0)
    forward(0)
    pass_on(1, 0, 0)
    w_step(0, 1)
    arrive(0, "b", "s")
    multiply(0, 1, 0)
    w_step(0, 2)
    arrive(0, "ap")
    multiply(0, 0, 1)
    multiply(0, 1, 1)
    w_step(1, 0)
    pass_on(0, 1, 0)
    w_step(0, 3)
    pass_on(0, 0, 1)
    pass_on(0, 1, 1)
    w_step(1, 1)
    collect(0, 0, 0)
    collect(1, 0, 0)
    w_deliver(0)
    forward(1)
    collect(0, 1, 0)
    w_step(1, 2)
    arrive(1, "b", "s")
    multiply(1, 1, 0)
    collect(0, 0, 1)
    arrive(1, "ap")
    multiply(1, 0, 1)
    multiply(1, 1, 1)
    w_step(2, 0)
    pass_on(1, 1, 0)
    collect(0, 1, 1)
    y_step(0, 0)
    w_step(1, 3)
    pass_on(1, 0, 1)
    pass_on(1, 1, 1)
    w_step(2, 1)
    y_step(0, 1)
    w_deliver(1)
    collect(1, 1, 0)
    collect(1, 0, 1)
    collect(1, 1, 1)
    y_step(1, 0)
    w_step(2, 2)
    y_step(0, 2)
    y_step(1, 1)
    w_step(2, 3)
    y_step(0, 3)
    y_step(1, 2)
    w_deliver(2)
    deliver(0)
    y_step(1, 3)
    deliver(1)
    receive(0)
    receive(1)

    for copy in sent:
        copy.wait_send()
    for pair in range(PAIRS):
        for part in range(2):

            @pl.when(jnp.logical_not(at_home & (zl == part)))
            def _():
                final_copy(pair, part).wait_send()
    for group in GROUPS:
        for pair, jb, ih in group:

            @pl.when(jnp.logical_not(rest_home & (src_jb == jb) & (ih == 0)))
            def _():
                rest_copy(pair, jb, ih).wait_send()


def cross(pair_table, image, view, embeddings):
    blocks = 4 * PAIRS
    dma = pltpu.SemaphoreType.DMA
    vmem = pl.BlockSpec(memory_space=pltpu.VMEM)
    return pl.pallas_call(
        cross_kernel,
        out_shape=jax.ShapeDtypeStruct((PAIRS, OWN, WIDTH), F32),
        in_specs=[pl.BlockSpec(memory_space=pltpu.SMEM), vmem, vmem, pl.BlockSpec(memory_space=pl.ANY)],
        out_specs=vmem,
        scratch_shapes=[
            pltpu.VMEM((STEPS * SLOTS, WIDTH), BF16),
            pltpu.VMEM((IMG_DEV, WIDTH), F32),
            pltpu.VMEM((IMG_DEV, 128), F32),
            pltpu.VMEM((PAIRS, 1, WIDTH), F32),
            pltpu.VMEM((PAIRS, IMG_DEV, WIDTH), BF16),
            pltpu.VMEM((PAIRS, WIDTH, IMG_DEV), BF16),
            pltpu.VMEM((PAIRS, STAT, WIDTH), F32),
            pltpu.VMEM((PAIRS, IMG_DEV, WIDTH), BF16),
            pltpu.VMEM((PAIRS, IMG_DEV, WIDTH), BF16),
            pltpu.VMEM((PAIRS, IMG_DEV, WIDTH), BF16),
            pltpu.VMEM((PAIRS, WIDTH, IMG_DEV), BF16),
            pltpu.VMEM((PAIRS, STAT, WIDTH), F32),
            pltpu.VMEM((PAIRS, 2, 2, STAT, WIDTH), F32),
            pltpu.VMEM((blocks, NX, 2, ROWS, WIDTH), F32),
            pltpu.VMEM((blocks, ROWS, WIDTH), F32),
            pltpu.VMEM((blocks, ROWS, WIDTH), F32),
            pltpu.VMEM((blocks, 2, ROWS, WIDTH), F32),
            pltpu.VMEM((blocks, 2, ROWS, WIDTH), F32),
            pltpu.VMEM((PAIRS, NY, ROWS, WIDTH), F32),
            pltpu.VMEM((PAIRS, 2, 4, ROWS, WIDTH), F32),
            pltpu.VMEM((PAIRS, 2, PART, WIDTH), F32),
            pltpu.VMEM((PAIRS, 2, PART, WIDTH), F32),
            *(pltpu.VMEM((NY, len(blocks_of), REST, WIDTH), F32) for blocks_of in GROUPS),
            *(pltpu.VMEM((2, 4, len(blocks_of), REST, WIDTH), F32) for blocks_of in GROUPS),
            pltpu.VMEM((blocks, REST, WIDTH), F32),
            pltpu.VMEM((PAIRS, NX, 2, REST, WIDTH), F32),
            dma((STEPS,)),
            dma((PAIRS, 5)),
            dma((PAIRS, 5)),
            dma((blocks, 6)),
            dma((blocks, 6)),
            dma((PAIRS, 2, 4)),
            dma((PAIRS, 2, 4)),
            dma((PAIRS, 2)),
            dma((PAIRS, 2)),
            dma((len(GROUPS), 2, 4)),
            dma((len(GROUPS), 2, 4)),
            dma((blocks,)),
            dma((PAIRS, NX, 2)),
        ],
        compiler_params=pltpu.CompilerParams(collective_id=0, has_side_effects=True),
        name="cross",
    )(pair_table, image, view, embeddings)


def local(embeddings, slot_image, slot_view, pair_table):
    shape = (STEPS * TILE, 128)
    block = cross(pair_table, slot_image.reshape(shape), slot_view.reshape(shape), embeddings)
    return jnp.swapaxes(block, 1, 2)


def solution(mesh):
    split = Mesh(mesh.devices.reshape(NY, NX, 2, 4, 2), AXES)
    placed = (P(DP, FEAT), P(DP), P(DP), P())
    return jax.shard_map(local, mesh=split, in_specs=placed, out_specs=P(None, FEAT, DP), check_vma=False)
```

```python
import jax
import jax.numpy as jnp
from jax import lax
from jax.experimental import pallas as pl
from jax.experimental.pallas import tpu as pltpu
from jax.sharding import Mesh
from jax.sharding import PartitionSpec as P

WIN = 2048
IMG_DEV = 512
PAIRS = 2
WIDTH = 256
OWN = 32
NX, NY = 4, 8
BLOCK = 64
STAT = 8
LEAD = 40
REST = BLOCK - LEAD
ROWS = LEAD + STAT
PART = OWN + STAT
CUT = 24
REST_CUT = 16
GROUPS = (
    ((0, 0, 0), (1, 0, 0)),
    ((0, 1, 0), (0, 0, 1), (0, 1, 1)),
    ((1, 1, 0), (1, 0, 1), (1, 1, 1)),
)
SLOTS = 1024
STEPS = 5
TILE = SLOTS // 128
VIEW_STRIDE = 16
AXES = ("y", "x", "zl", "zh", "core")
FEAT = ("zh", "core")
DP = ("y", "x", "zl")
EPS = 1e-05
F32 = jnp.float32
BF16 = jnp.bfloat16
MESH = pl.DeviceIdType.MESH


def place_of(plane, core, jb, ih, half):
    ahead = (1 - jb) * (ih * half + (1 - ih) * (7 - 5 * half)) + jb * (4 + 2 * ih - half)
    return (2 * plane + core + NY + (1 - 2 * (plane % 2)) * ahead) % NY


def cross_kernel(
    pair_ref, image_ref, view_ref, emb_ref, out_ref,
    emb, acc, found, counts, x1_ref, x2_ref, stat_ref,
    x1p, x1a, x1ap, x2b, statb, x1stat, cb, relay_p, relay_m, from_m, from_p, total, yr, fs, fr,
    w0, w1, w2, v0, v1, v2, rest, rest_in,
    emb_sem, z_send, z_recv, x_send, x_recv, y_send, y_recv, f_send, f_recv, w_send, w_recv, r_send, r_recv,
):
    y, x, zl, h, core = [lax.axis_index(axis) for axis in AXES]
    plane_a = h + 1 - 2 * (h % 2)
    plane_b = 3 - h
    other = 1 - core
    xp, xa, xm = (x + 1) % NX, (x + 2) % NX, (x + 3) % NX
    yp, ym = (y + 1) % NY, (y + NY - 1) % NY
    yp2, ym2 = (y + 2) % NY, (y + NY - 2) % NY

    mine = (2 * NY + (1 - 2 * (h % 2)) * (y - 2 * h - core)) % NY
    jb = ((mine + 1) // 4) % 2
    ih = ((mine < 2) | ((mine > 4) & (mine < 7))).astype(jnp.int32)
    half = (((mine > 0) & (mine < 4)) | (mine == 5)).astype(jnp.int32)
    owner_y = 2 * (h + jb * (3 - 2 * h)) + core
    owner_h = h + ih * (1 - 2 * (h % 2))
    at_home = (owner_y == y) & (owner_h == h) & (half == core)
    jh, src_core = y // 2, y % 2
    src_jb = (jh // 2 + h // 2) % 2
    src_h = jh + src_jb * (3 - 2 * jh)
    src_ih = (src_h + h) % 2
    src_y = place_of(src_h, src_core, src_jb, src_ih, core)
    rest_y = 2 * x + core
    rest_home = (rest_y == y) & (src_h == h) & (zl == 1)

    loads = []
    for step in range(STEPS):
        rows = slice(step * SLOTS, (step + 1) * SLOTS)
        loads.append(pltpu.make_async_copy(emb_ref.at[rows], emb.at[rows], emb_sem.at[step]))
        loads[-1].start()

    barrier = pltpu.get_barrier_semaphore()
    for peer in ({"x": xp}, {"x": xm}, {"y": yp}, {"y": ym}, {"y": yp2}, {"y": ym2}, {"zh": plane_a}, {"zh": plane_b}, {"core": other}):
        pl.semaphore_signal(barrier, inc=1, device_id=peer, device_id_type=MESH)
    for part in range(2):

        @pl.when(jnp.logical_not(at_home & (zl == part)))
        def _():
            pl.semaphore_signal(
                barrier,
                inc=1,
                device_id={"y": src_y, "zl": part, "zh": src_h, "core": src_core},
                device_id_type=MESH,
            )

    for from_x in range(NX):
        for part in range(2):

            @pl.when((zl == 1) & jnp.logical_not(rest_home & (x == from_x) & (zl == part)))
            def _():
                pl.semaphore_signal(
                    barrier,
                    inc=1,
                    device_id={"y": rest_y, "x": from_x, "zl": part, "zh": src_h, "core": src_core},
                    device_id_type=MESH,
                )

    sent = []

    def send(src, dst, send_sem, recv_sem, peer):
        copy = pltpu.make_async_remote_copy(
            src_ref=src, dst_ref=dst, send_sem=send_sem, recv_sem=recv_sem, device_id=peer, device_id_type=MESH
        )
        copy.start()
        sent.append(copy)
        return copy

    z = {}

    def offer(pair, name):
        slot, src, dst, peer = {
            "p": (0, x1_ref, x1p, {"core": other}),
            "b": (1, x2_ref, x2b, {"zh": plane_b}),
            "s": (2, stat_ref, statb, {"zh": plane_b}),
            "a": (3, x1_ref, x1a, {"zh": plane_a}),
        }[name]
        z[name, pair] = send(src.at[pair], dst.at[pair], z_send.at[pair, slot], z_recv.at[pair, slot], peer)

    def arrive(pair, *names):
        for name in names:
            z[name, pair].wait_recv()

    base = (y * NX * 2 + x * 2 + zl) * IMG_DEV
    wanted = (lax.broadcasted_iota(jnp.int32, (IMG_DEV, 128), 0) + base) * VIEW_STRIDE

    def pick(pair, side):
        target = wanted + pair_ref[pair, side]
        second = wanted + pair_ref[pair, 1]
        acc[...] = jnp.zeros_like(acc)
        if side == 0:
            found[...] = jnp.zeros_like(found)

        def step(index, carry):
            key = image_ref[pl.ds(pl.multiple_of(index * TILE, TILE), TILE), :] * VIEW_STRIDE
            key += view_ref[pl.ds(pl.multiple_of(index * TILE, TILE), TILE), :]
            keys = [key[row : row + 1, :] for row in range(TILE)]
            chosen = jnp.concatenate([jnp.where(one == target, 1.0, 0.0).astype(BF16) for one in keys], axis=1)
            rows = emb[pl.ds(pl.multiple_of(index * SLOTS, SLOTS), SLOTS), :]
            acc[...] += jnp.dot(chosen, rows, preferred_element_type=F32)
            if side == 0:
                hits = [jnp.where(one == second, 1.0, 0.0) for one in keys]
                found[...] += sum(hits[1:], hits[0])
            return carry

        lax.fori_loop(0, STEPS, step, 0)

    def pick_first(pair):
        pick(pair, 0)
        present = jnp.sum(found[...], axis=1, keepdims=True)
        x1_ref[pair] = jnp.where(present > 0.5, acc[...], 0.0).astype(BF16)
        counts[pair] = jnp.broadcast_to(jnp.sum(present, axis=0, keepdims=True), (1, WIDTH))

    def pick_second(pair):
        pick(pair, 1)
        row = lax.broadcasted_iota(jnp.int32, (STAT, WIDTH), 0)
        rows = acc[...]
        x2_ref[pair] = rows.T.astype(BF16)
        plain = jnp.sum(rows, axis=0, keepdims=True)
        square = jnp.sum(rows * rows, axis=0, keepdims=True)
        stat_ref[pair] = jnp.where(
            row == 2, plain, jnp.where(row == 3, square, jnp.where(row == 4, counts[pair], 0.0))
        )

    def forward(pair):
        arrive(pair, "a")
        z["ap", pair] = send(
            x1a.at[pair], x1ap.at[pair], z_send.at[pair, 4], z_recv.at[pair, 4], {"core": other}
        )

    stats_done = set()
    xc = {}

    def block_of(pair, jb, ih):
        return 4 * pair + 2 * jb + ih

    def multiply(pair, jb, ih):
        k = block_of(pair, jb, ih)
        group, place = next(
            (g, blocks.index((pair, jb, ih))) for g, blocks in enumerate(GROUPS) if (pair, jb, ih) in blocks
        )
        second = (x2b if jb else x2_ref)[pair]
        stat = (statb if jb else stat_ref)[pair]
        row = lax.broadcasted_iota(jnp.int32, (STAT, WIDTH), 0)
        for slot, (ref, half) in enumerate((((x1a if ih else x1_ref), core), ((x1ap if ih else x1p), other))):
            first = ref[pair]
            if (pair, ih, slot) not in stats_done:
                stats_done.add((pair, ih, slot))
                wide = first.astype(F32)
                plain = jnp.sum(wide, axis=0, keepdims=True)
                square = jnp.sum(wide * wide, axis=0, keepdims=True)
                x1stat[pair, ih, slot] = jnp.where(row == 0, plain, jnp.where(row == 1, square, 0.0))
            product = jnp.dot(second, first, preferred_element_type=F32)
            sums = x1stat[pair, ih, slot] + stat
            for dest in range(NX):
                cb[k, dest, half, 0:LEAD] = product[dest * BLOCK : dest * BLOCK + LEAD]
                cb[k, dest, half, LEAD:ROWS] = sums
                w[group][2 * dest + half, place] = product[dest * BLOCK + LEAD : (dest + 1) * BLOCK]
        for slot, (src, dst, to) in enumerate(
            (
                (cb.at[k, xa, 0], relay_p.at[k], xp),
                (cb.at[k, xa, 1], relay_m.at[k], xm),
                (cb.at[k, xp, 1], from_m.at[k, 1], xp),
                (cb.at[k, xm, 0], from_p.at[k, 0], xm),
            )
        ):
            xc[k, slot] = send(src, dst, x_send.at[k, slot], x_recv.at[k, slot], {"x": to})

    def pass_on(pair, jb, ih):
        k = block_of(pair, jb, ih)
        xc[k, 0].wait_recv()
        cb[k, xp, 0] += relay_p[k]
        xc[k, 4] = send(cb.at[k, xp, 0], from_m.at[k, 0], x_send.at[k, 4], x_recv.at[k, 4], {"x": xp})
        xc[k, 1].wait_recv()
        cb[k, xm, 1] += relay_m[k]
        xc[k, 5] = send(cb.at[k, xm, 1], from_p.at[k, 1], x_send.at[k, 5], x_recv.at[k, 5], {"x": xm})

    def collect(pair, jb, ih):
        k = block_of(pair, jb, ih)
        for slot in (2, 3, 4, 5):
            xc[k, slot].wait_recv()
        for half in range(2):
            total[pair, place_of(h, core, jb, ih, half)] = cb[k, x, half] + from_m[k, half] + from_p[k, half]

    def y_ways(key, copies, part, landing, send_sem, recv_sem, cut, step):
        for way in range(2):
            one, two = (ym, ym2) if way else (yp, yp2)
            rows = slice(cut, None) if way else slice(0, cut)

            def at(distance):
                return (y + (NY - distance if way else distance)) % NY

            def go(slot, src, dst, to):
                copies[key, way, slot] = send(src, dst, send_sem(way, slot), recv_sem(way, slot), {"y": to})

            if step == 0:
                far = part(at(4), rows)
                go(0, far, landing(way, 0, slice(0, far.shape[-2])), two)
                go(1, part(at(3)), landing(way, 1), one)
                go(2, part(at(1)), landing(way, 2), one)
                continue
            copies[key, way, 0].wait_recv()
            copies[key, way, 1].wait_recv()
            second = part(at(2))
            second[...] += landing(way, 1)[...]
            half_of = part(at(2), rows)
            half_of[...] += landing(way, 0, slice(0, half_of.shape[-2]))[...]
            go(3, second, landing(way, 3), two)

    yc = {}

    def y_step(pair, step):
        y_ways(
            pair,
            yc,
            lambda place, rows=slice(0, ROWS): total.at[pair, place, slice(rows.start, rows.stop or ROWS)],
            lambda way, slot, rows=slice(0, ROWS): yr.at[pair, way, slot, rows],
            lambda way, slot: y_send.at[pair, way, slot],
            lambda way, slot: y_recv.at[pair, way, slot],
            CUT,
            step,
        )

    w, v = (w0, w1, w2), (v0, v1, v2)
    wc = {}

    def w_step(group, step):
        y_ways(
            group,
            wc,
            lambda place, rows=slice(0, REST): w[group].at[place, :, slice(rows.start, rows.stop or REST)],
            lambda way, slot, rows=slice(0, REST): v[group].at[way, slot, :, rows],
            lambda way, slot: w_send.at[group, way, slot],
            lambda way, slot: w_recv.at[group, way, slot],
            REST_CUT,
            step,
        )

    def rest_copy(pair, jb, ih):
        k = block_of(pair, jb, ih)
        return pltpu.make_async_remote_copy(
            src_ref=rest.at[k],
            dst_ref=rest_in.at[pair, x, zl],
            send_sem=r_send.at[k],
            recv_sem=r_recv.at[pair, x, zl],
            device_id={
                "y": 2 * (plane_b if jb else h) + core,
                "x": y // 2,
                "zl": 1,
                "zh": plane_a if ih else h,
                "core": y % 2,
            },
            device_id_type=MESH,
        )

    def w_deliver(group):
        for way in range(2):
            wc[group, way, 2].wait_recv()
            wc[group, way, 3].wait_recv()
        for place, (pair, jb, ih) in enumerate(GROUPS[group]):
            k = block_of(pair, jb, ih)
            near = v[group][0, 2, place] + v[group][1, 2, place]
            rest[k] = w[group][y, place] + near + (v[group][0, 3, place] + v[group][1, 3, place])
            if ih:
                rest_copy(pair, jb, ih).start()
                continue
            same = rest_home & (src_jb == jb)

            @pl.when(same)
            def _():
                rest_in[pair, x, zl] = rest[k]

            @pl.when(jnp.logical_not(same))
            def _():
                rest_copy(pair, jb, ih).start()

    def rest_receive(pair):
        @pl.when(zl == 1)
        def _():
            for from_x in range(NX):
                for part in range(2):

                    @pl.when(jnp.logical_not(rest_home & (x == from_x) & (zl == part)))
                    def _():
                        pltpu.make_async_remote_copy(
                            src_ref=rest.at[0],
                            dst_ref=rest_in.at[pair, from_x, part],
                            send_sem=r_send.at[0],
                            recv_sem=r_recv.at[pair, from_x, part],
                            device_id={"x": xp},
                            device_id_type=MESH,
                        ).wait_recv()

            lead = OWN - REST
            summed = rest_in[pair, 0, 0]
            for slot in range(1, 2 * NX):
                summed += rest_in[pair, slot // 2, slot % 2]
            fr[pair, 0, lead:OWN] += summed

    def deliver(pair):
        for way in range(2):
            yc[pair, way, 2].wait_recv()
            yc[pair, way, 3].wait_recv()
        done = total[pair, y] + (yr[pair, 0, 2] + yr[pair, 1, 2]) + (yr[pair, 0, 3] + yr[pair, 1, 3])
        for part in range(2):
            if part:
                fs[pair, 1, 0 : LEAD - OWN] = done[OWN:LEAD]
                fs[pair, 1, LEAD - OWN : OWN] = jnp.zeros((REST, WIDTH), F32)
            else:
                fs[pair, 0, 0:OWN] = done[0:OWN]
            fs[pair, part, OWN:PART] = done[LEAD:ROWS]
            same = at_home & (zl == part)

            @pl.when(same)
            def _():
                fr[pair, zl] = fs[pair, part]

            @pl.when(jnp.logical_not(same))
            def _():
                final_copy(pair, part).start()

    def final_copy(pair, part):
        return pltpu.make_async_remote_copy(
            src_ref=fs.at[pair, part],
            dst_ref=fr.at[pair, zl],
            send_sem=f_send.at[pair, part],
            recv_sem=f_recv.at[pair, zl],
            device_id={"y": owner_y, "zl": part, "zh": owner_h, "core": half},
            device_id_type=MESH,
        )

    def receive(pair):
        for part in range(2):

            @pl.when(jnp.logical_not(at_home & (zl == part)))
            def _():
                pltpu.make_async_remote_copy(
                    src_ref=fs.at[pair, part],
                    dst_ref=fr.at[pair, part],
                    send_sem=f_send.at[pair, part],
                    recv_sem=f_recv.at[pair, part],
                    device_id={"y": owner_y, "zl": part, "zh": owner_h, "core": half},
                    device_id_type=MESH,
                ).wait_recv()

        rest_receive(pair)
        both = fr[pair, 0] + fr[pair, 1]
        count = both[OWN + 4 : OWN + 5, 0:1]
        lane = lax.broadcasted_iota(jnp.int32, (OWN, WIDTH), 1)
        row = lax.broadcasted_iota(jnp.int32, (OWN, WIDTH), 0)
        own = lane == row + (x * BLOCK + zl * OWN)

        def column(line):
            return jnp.sum(jnp.where(own, line, 0.0), axis=1, keepdims=True)

        mean_first = both[OWN : OWN + 1] / count
        square_first = both[OWN + 1 : OWN + 2] / count
        mean_second = column(both[OWN + 2 : OWN + 3]) / count
        square_second = column(both[OWN + 3 : OWN + 4]) / count
        spread_first = jnp.sqrt(square_first - mean_first * mean_first + EPS)
        spread_second = jnp.sqrt(square_second - mean_second * mean_second + EPS)
        out_ref[pair] = (both[0:OWN] / count - mean_second * mean_first) / (spread_second * spread_first)

    def enter():
        pl.semaphore_wait(barrier, 15 - at_home.astype(jnp.int32) - rest_home.astype(jnp.int32))

    for load in loads:
        load.wait()
    pick_first(0)
    enter()
    offer(0, "a")
    offer(0, "p")
    pick_second(0)
    offer(0, "b")
    offer(0, "s")
    pick_first(1)
    offer(1, "a")
    offer(1, "p")
    pick_second(1)
    offer(1, "b")
    offer(1, "s")
    arrive(1, "p")
    multiply(1, 0, 0)
    arrive(0, "p")
    multiply(0, 0, 0)
    w_step(0, 0)
    pass_on(1, 0, 0)
    forward(0)
    pass_on(0, 0, 0)
    w_step(0, 1)
    arrive(0, "ap")
    multiply(0, 0, 1)
    arrive(0, "b", "s")
    multiply(0, 1, 0)
    multiply(0, 1, 1)
    collect(0, 0, 0)
    collect(1, 0, 0)
    w_step(1, 0)
    pass_on(0, 0, 1)
    w_deliver(0)
    pass_on(0, 1, 0)
    forward(1)
    pass_on(0, 1, 1)
    w_step(1, 1)
    arrive(1, "ap")
    multiply(1, 0, 1)
    arrive(1, "b", "s")
    multiply(1, 1, 0)
    multiply(1, 1, 1)
    w_step(2, 0)
    collect(0, 1, 0)
    collect(0, 1, 1)
    collect(0, 0, 1)
    y_step(0, 0)
    pass_on(1, 0, 1)
    w_deliver(1)
    pass_on(1, 1, 0)
    pass_on(1, 1, 1)
    w_step(2, 1)
    collect(1, 0, 1)
    collect(1, 1, 0)
    collect(1, 1, 1)
    y_step(1, 0)
    y_step(0, 1)
    w_deliver(2)
    y_step(1, 1)
    deliver(0)
    deliver(1)
    receive(0)
    receive(1)

    for copy in sent:
        copy.wait_send()
    for pair in range(PAIRS):
        for part in range(2):

            @pl.when(jnp.logical_not(at_home & (zl == part)))
            def _():
                final_copy(pair, part).wait_send()
    for group in GROUPS:
        for pair, jb, ih in group:

            @pl.when(jnp.logical_not(rest_home & (src_jb == jb) & (ih == 0)))
            def _():
                rest_copy(pair, jb, ih).wait_send()


def cross(pair_table, image, view, embeddings):
    blocks = 4 * PAIRS
    dma = pltpu.SemaphoreType.DMA
    vmem = pl.BlockSpec(memory_space=pltpu.VMEM)
    return pl.pallas_call(
        cross_kernel,
        out_shape=jax.ShapeDtypeStruct((PAIRS, OWN, WIDTH), F32),
        in_specs=[pl.BlockSpec(memory_space=pltpu.SMEM), vmem, vmem, pl.BlockSpec(memory_space=pl.ANY)],
        out_specs=vmem,
        scratch_shapes=[
            pltpu.VMEM((STEPS * SLOTS, WIDTH), BF16),
            pltpu.VMEM((IMG_DEV, WIDTH), F32),
            pltpu.VMEM((IMG_DEV, 128), F32),
            pltpu.VMEM((PAIRS, 1, WIDTH), F32),
            pltpu.VMEM((PAIRS, IMG_DEV, WIDTH), BF16),
            pltpu.VMEM((PAIRS, WIDTH, IMG_DEV), BF16),
            pltpu.VMEM((PAIRS, STAT, WIDTH), F32),
            pltpu.VMEM((PAIRS, IMG_DEV, WIDTH), BF16),
            pltpu.VMEM((PAIRS, IMG_DEV, WIDTH), BF16),
            pltpu.VMEM((PAIRS, IMG_DEV, WIDTH), BF16),
            pltpu.VMEM((PAIRS, WIDTH, IMG_DEV), BF16),
            pltpu.VMEM((PAIRS, STAT, WIDTH), F32),
            pltpu.VMEM((PAIRS, 2, 2, STAT, WIDTH), F32),
            pltpu.VMEM((blocks, NX, 2, ROWS, WIDTH), F32),
            pltpu.VMEM((blocks, ROWS, WIDTH), F32),
            pltpu.VMEM((blocks, ROWS, WIDTH), F32),
            pltpu.VMEM((blocks, 2, ROWS, WIDTH), F32),
            pltpu.VMEM((blocks, 2, ROWS, WIDTH), F32),
            pltpu.VMEM((PAIRS, NY, ROWS, WIDTH), F32),
            pltpu.VMEM((PAIRS, 2, 4, ROWS, WIDTH), F32),
            pltpu.VMEM((PAIRS, 2, PART, WIDTH), F32),
            pltpu.VMEM((PAIRS, 2, PART, WIDTH), F32),
            *(pltpu.VMEM((NY, len(blocks_of), REST, WIDTH), F32) for blocks_of in GROUPS),
            *(pltpu.VMEM((2, 4, len(blocks_of), REST, WIDTH), F32) for blocks_of in GROUPS),
            pltpu.VMEM((blocks, REST, WIDTH), F32),
            pltpu.VMEM((PAIRS, NX, 2, REST, WIDTH), F32),
            dma((STEPS,)),
            dma((PAIRS, 5)),
            dma((PAIRS, 5)),
            dma((blocks, 6)),
            dma((blocks, 6)),
            dma((PAIRS, 2, 4)),
            dma((PAIRS, 2, 4)),
            dma((PAIRS, 2)),
            dma((PAIRS, 2)),
            dma((len(GROUPS), 2, 4)),
            dma((len(GROUPS), 2, 4)),
            dma((blocks,)),
            dma((PAIRS, NX, 2)),
        ],
        compiler_params=pltpu.CompilerParams(collective_id=0, has_side_effects=True),
        name="cross",
    )(pair_table, image, view, embeddings)


def local(embeddings, slot_image, slot_view, pair_table):
    shape = (STEPS * TILE, 128)
    block = cross(pair_table, slot_image.reshape(shape), slot_view.reshape(shape), embeddings)
    return jnp.swapaxes(block, 1, 2)


def solution(mesh):
    split = Mesh(mesh.devices.reshape(NY, NX, 2, 4, 2), AXES)
    placed = (P(DP, FEAT), P(DP), P(DP), P())
    return jax.shard_map(local, mesh=split, in_specs=placed, out_specs=P(None, FEAT, DP), check_vma=False)
```

```python
import jax
import jax.numpy as jnp
from jax import lax
from jax.experimental import pallas as pl
from jax.experimental.pallas import tpu as pltpu
from jax.sharding import Mesh
from jax.sharding import PartitionSpec as P

WIN = 2048
IMG_DEV = 512
PAIRS = 2
WIDTH = 256
OWN = 32
NX, NY = 4, 8
BLOCK = 64
STAT = 8
LEAD = 40
REST = BLOCK - LEAD
ROWS = LEAD + STAT
PART = OWN + STAT
CUT = 24
REST_CUT = 16
GROUPS = (
    ((0, 0, 0), (1, 0, 0)),
    ((0, 1, 0), (0, 0, 1), (0, 1, 1)),
    ((1, 1, 0), (1, 0, 1), (1, 1, 1)),
)
SLOTS = 1024
STEPS = 5
TILE = SLOTS // 128
VIEW_STRIDE = 16
AXES = ("y", "x", "zl", "zh", "core")
FEAT = ("zh", "core")
DP = ("y", "x", "zl")
EPS = 1e-05
F32 = jnp.float32
BF16 = jnp.bfloat16
MESH = pl.DeviceIdType.MESH


def place_of(plane, core, jb, ih, half):
    ahead = (1 - jb) * (ih * half + (1 - ih) * (7 - 5 * half)) + jb * (4 + 2 * ih - half)
    return (2 * plane + core + NY + (1 - 2 * (plane % 2)) * ahead) % NY


def cross_kernel(
    pair_ref, image_ref, view_ref, emb_ref, out_ref,
    emb, acc, found, counts, x1_ref, x2_ref, stat_ref,
    x1p, x1a, x1ap, x2b, statb, x1stat, cb, relay_p, relay_m, from_m, from_p, total, yr, fs, fr,
    w0, w1, w2, v0, v1, v2, rest, rest_in, u0, u1, u2, g0, g1, g2,
    emb_sem, z_send, z_recv, x_send, x_recv, y_send, y_recv, f_send, f_recv, w_send, w_recv, r_send, r_recv, g_send, g_recv,
):
    y, x, zl, h, core = [lax.axis_index(axis) for axis in AXES]
    plane_a = h + 1 - 2 * (h % 2)
    plane_b = 3 - h
    other = 1 - core
    xp, xa, xm = (x + 1) % NX, (x + 2) % NX, (x + 3) % NX
    yp, ym = (y + 1) % NY, (y + NY - 1) % NY
    yp2, ym2 = (y + 2) % NY, (y + NY - 2) % NY

    mine = (2 * NY + (1 - 2 * (h % 2)) * (y - 2 * h - core)) % NY
    jb = ((mine + 1) // 4) % 2
    ih = ((mine < 2) | ((mine > 4) & (mine < 7))).astype(jnp.int32)
    half = (((mine > 0) & (mine < 4)) | (mine == 5)).astype(jnp.int32)
    owner_y = 2 * (h + jb * (3 - 2 * h)) + core
    owner_h = h + ih * (1 - 2 * (h % 2))
    at_home = (owner_y == y) & (owner_h == h) & (half == core)
    jh, src_core = y // 2, y % 2
    src_jb = (jh // 2 + h // 2) % 2
    src_h = jh + src_jb * (3 - 2 * jh)
    src_ih = (src_h + h) % 2
    src_y = place_of(src_h, src_core, src_jb, src_ih, core)
    rest_y = 2 * x + core
    rest_home = (rest_y == y) & (src_h == h) & (zl == 1)
    hub = y // 2
    at_hub = x == hub

    loads = []
    for step in range(STEPS):
        rows = slice(step * SLOTS, (step + 1) * SLOTS)
        loads.append(pltpu.make_async_copy(emb_ref.at[rows], emb.at[rows], emb_sem.at[step]))
        loads[-1].start()

    barrier = pltpu.get_barrier_semaphore()
    for peer in ({"x": xp}, {"x": xm}, {"x": xa}, {"y": yp}, {"y": ym}, {"y": yp2}, {"y": ym2}, {"zh": plane_a}, {"zh": plane_b}, {"core": other}):
        pl.semaphore_signal(barrier, inc=1, device_id=peer, device_id_type=MESH)
    for part in range(2):

        @pl.when(jnp.logical_not(at_home & (zl == part)))
        def _():
            pl.semaphore_signal(
                barrier,
                inc=1,
                device_id={"y": src_y, "zl": part, "zh": src_h, "core": src_core},
                device_id_type=MESH,
            )

    for part in range(2):

        @pl.when((zl == 1) & jnp.logical_not(rest_home & (zl == part)))
        def _():
            pl.semaphore_signal(
                barrier,
                inc=1,
                device_id={"y": rest_y, "zl": part, "zh": src_h, "core": src_core},
                device_id_type=MESH,
            )

    sent = []

    def send(src, dst, send_sem, recv_sem, peer):
        copy = pltpu.make_async_remote_copy(
            src_ref=src, dst_ref=dst, send_sem=send_sem, recv_sem=recv_sem, device_id=peer, device_id_type=MESH
        )
        copy.start()
        sent.append(copy)
        return copy

    z = {}

    def offer(pair, name):
        slot, src, dst, peer = {
            "p": (0, x1_ref, x1p, {"core": other}),
            "b": (1, x2_ref, x2b, {"zh": plane_b}),
            "s": (2, stat_ref, statb, {"zh": plane_b}),
            "a": (3, x1_ref, x1a, {"zh": plane_a}),
        }[name]
        z[name, pair] = send(src.at[pair], dst.at[pair], z_send.at[pair, slot], z_recv.at[pair, slot], peer)

    def arrive(pair, *names):
        for name in names:
            z[name, pair].wait_recv()

    base = (y * NX * 2 + x * 2 + zl) * IMG_DEV
    wanted = (lax.broadcasted_iota(jnp.int32, (IMG_DEV, 128), 0) + base) * VIEW_STRIDE

    def pick(pair, side):
        target = wanted + pair_ref[pair, side]
        second = wanted + pair_ref[pair, 1]
        acc[...] = jnp.zeros_like(acc)
        if side == 0:
            found[...] = jnp.zeros_like(found)

        def step(index, carry):
            key = image_ref[pl.ds(pl.multiple_of(index * TILE, TILE), TILE), :] * VIEW_STRIDE
            key += view_ref[pl.ds(pl.multiple_of(index * TILE, TILE), TILE), :]
            keys = [key[row : row + 1, :] for row in range(TILE)]
            chosen = jnp.concatenate([jnp.where(one == target, 1.0, 0.0).astype(BF16) for one in keys], axis=1)
            rows = emb[pl.ds(pl.multiple_of(index * SLOTS, SLOTS), SLOTS), :]
            acc[...] += jnp.dot(chosen, rows, preferred_element_type=F32)
            if side == 0:
                hits = [jnp.where(one == second, 1.0, 0.0) for one in keys]
                found[...] += sum(hits[1:], hits[0])
            return carry

        lax.fori_loop(0, STEPS, step, 0)

    def pick_first(pair):
        pick(pair, 0)
        present = jnp.sum(found[...], axis=1, keepdims=True)
        x1_ref[pair] = jnp.where(present > 0.5, acc[...], 0.0).astype(BF16)
        counts[pair] = jnp.broadcast_to(jnp.sum(present, axis=0, keepdims=True), (1, WIDTH))

    def pick_second(pair):
        pick(pair, 1)
        row = lax.broadcasted_iota(jnp.int32, (STAT, WIDTH), 0)
        rows = acc[...]
        x2_ref[pair] = rows.T.astype(BF16)
        plain = jnp.sum(rows, axis=0, keepdims=True)
        square = jnp.sum(rows * rows, axis=0, keepdims=True)
        stat_ref[pair] = jnp.where(
            row == 2, plain, jnp.where(row == 3, square, jnp.where(row == 4, counts[pair], 0.0))
        )

    def forward(pair):
        arrive(pair, "a")
        z["ap", pair] = send(
            x1a.at[pair], x1ap.at[pair], z_send.at[pair, 4], z_recv.at[pair, 4], {"core": other}
        )

    stats_done = set()
    xc = {}

    def block_of(pair, jb, ih):
        return 4 * pair + 2 * jb + ih

    def multiply(pair, jb, ih):
        k = block_of(pair, jb, ih)
        group, place = next(
            (g, blocks.index((pair, jb, ih))) for g, blocks in enumerate(GROUPS) if (pair, jb, ih) in blocks
        )
        second = (x2b if jb else x2_ref)[pair]
        stat = (statb if jb else stat_ref)[pair]
        row = lax.broadcasted_iota(jnp.int32, (STAT, WIDTH), 0)
        for slot, (ref, half) in enumerate((((x1a if ih else x1_ref), core), ((x1ap if ih else x1p), other))):
            first = ref[pair]
            if (pair, ih, slot) not in stats_done:
                stats_done.add((pair, ih, slot))
                wide = first.astype(F32)
                plain = jnp.sum(wide, axis=0, keepdims=True)
                square = jnp.sum(wide * wide, axis=0, keepdims=True)
                x1stat[pair, ih, slot] = jnp.where(row == 0, plain, jnp.where(row == 1, square, 0.0))
            product = jnp.dot(second, first, preferred_element_type=F32)
            sums = x1stat[pair, ih, slot] + stat
            for dest in range(NX):
                cb[k, dest, half, 0:LEAD] = product[dest * BLOCK : dest * BLOCK + LEAD]
                cb[k, dest, half, LEAD:ROWS] = sums
                w[group][2 * dest + half, place] = product[dest * BLOCK + LEAD : (dest + 1) * BLOCK]
        for slot, (src, dst, to) in enumerate(
            (
                (cb.at[k, xa, 0], relay_p.at[k], xp),
                (cb.at[k, xa, 1], relay_m.at[k], xm),
                (cb.at[k, xp, 1], from_m.at[k, 1], xp),
                (cb.at[k, xm, 0], from_p.at[k, 0], xm),
            )
        ):
            xc[k, slot] = send(src, dst, x_send.at[k, slot], x_recv.at[k, slot], {"x": to})

    def pass_on(pair, jb, ih):
        k = block_of(pair, jb, ih)
        xc[k, 0].wait_recv()
        cb[k, xp, 0] += relay_p[k]
        xc[k, 4] = send(cb.at[k, xp, 0], from_m.at[k, 0], x_send.at[k, 4], x_recv.at[k, 4], {"x": xp})
        xc[k, 1].wait_recv()
        cb[k, xm, 1] += relay_m[k]
        xc[k, 5] = send(cb.at[k, xm, 1], from_p.at[k, 1], x_send.at[k, 5], x_recv.at[k, 5], {"x": xm})

    def collect(pair, jb, ih):
        k = block_of(pair, jb, ih)
        for slot in (2, 3, 4, 5):
            xc[k, slot].wait_recv()
        for half in range(2):
            total[pair, place_of(h, core, jb, ih, half)] = cb[k, x, half] + from_m[k, half] + from_p[k, half]

    def y_ways(key, copies, part, landing, send_sem, recv_sem, cut, step):
        for way in range(2):
            one, two = (ym, ym2) if way else (yp, yp2)
            rows = slice(cut, None) if way else slice(0, cut)

            def at(distance):
                return (y + (NY - distance if way else distance)) % NY

            def go(slot, src, dst, to):
                copies[key, way, slot] = send(src, dst, send_sem(way, slot), recv_sem(way, slot), {"y": to})

            if step == 0:
                far = part(at(4), rows)
                go(0, far, landing(way, 0, slice(0, far.shape[-2])), two)
                go(1, part(at(3)), landing(way, 1), one)
                go(2, part(at(1)), landing(way, 2), one)
                continue
            copies[key, way, 0].wait_recv()
            copies[key, way, 1].wait_recv()
            second = part(at(2))
            second[...] += landing(way, 1)[...]
            half_of = part(at(2), rows)
            half_of[...] += landing(way, 0, slice(0, half_of.shape[-2]))[...]
            go(3, second, landing(way, 3), two)

    yc = {}

    def y_step(pair, step):
        y_ways(
            pair,
            yc,
            lambda place, rows=slice(0, ROWS): total.at[pair, place, slice(rows.start, rows.stop or ROWS)],
            lambda way, slot, rows=slice(0, ROWS): yr.at[pair, way, slot, rows],
            lambda way, slot: y_send.at[pair, way, slot],
            lambda way, slot: y_recv.at[pair, way, slot],
            CUT,
            step,
        )

    w, v = (w0, w1, w2), (v0, v1, v2)
    wc = {}

    def w_step(group, step):
        y_ways(
            group,
            wc,
            lambda place, rows=slice(0, REST): w[group].at[place, :, slice(rows.start, rows.stop or REST)],
            lambda way, slot, rows=slice(0, REST): v[group].at[way, slot, :, rows],
            lambda way, slot: w_send.at[group, way, slot],
            lambda way, slot: w_recv.at[group, way, slot],
            REST_CUT,
            step,
        )

    def rest_copy(pair, jb, ih):
        k = block_of(pair, jb, ih)
        return pltpu.make_async_remote_copy(
            src_ref=rest.at[k],
            dst_ref=rest_in.at[pair, zl],
            send_sem=r_send.at[k],
            recv_sem=r_recv.at[pair, zl],
            device_id={
                "y": 2 * (plane_b if jb else h) + core,
                "x": hub,
                "zl": 1,
                "zh": plane_a if ih else h,
                "core": y % 2,
            },
            device_id_type=MESH,
        )

    u, gx = (u0, u1, u2), (g0, g1, g2)

    def gather_copy(group, from_x, to=hub):
        return pltpu.make_async_remote_copy(
            src_ref=u[group],
            dst_ref=gx[group].at[from_x],
            send_sem=g_send.at[group],
            recv_sem=g_recv.at[group, from_x],
            device_id={"x": to},
            device_id_type=MESH,
        )

    def w_gather(group):
        for way in range(2):
            wc[group, way, 2].wait_recv()
            wc[group, way, 3].wait_recv()
        near = v[group][0, 2] + v[group][1, 2]
        u[group][...] = w[group][y] + near + (v[group][0, 3] + v[group][1, 3])

        @pl.when(jnp.logical_not(at_hub))
        def _():
            gather_copy(group, x).start()

    def w_deliver(group):
        @pl.when(at_hub)
        def _():
            for from_x in range(NX):

                @pl.when(x != from_x)
                def _():
                    gather_copy(group, from_x, xp).wait_recv()

            summed = u[group][...] + gx[group][xa] + (gx[group][xp] + gx[group][xm])
            for place, (pair, jb, ih) in enumerate(GROUPS[group]):
                rest[block_of(pair, jb, ih)] = summed[place]
            for pair, jb, ih in GROUPS[group]:
                if ih:
                    rest_copy(pair, jb, ih).start()
                    continue
                same = rest_home & (src_jb == jb)

                @pl.when(same)
                def _():
                    rest_in[pair, zl] = rest[block_of(pair, jb, ih)]

                @pl.when(jnp.logical_not(same))
                def _():
                    rest_copy(pair, jb, ih).start()

    def rest_receive(pair):
        @pl.when(zl == 1)
        def _():
            for part in range(2):

                @pl.when(jnp.logical_not(rest_home & (zl == part)))
                def _():
                    pltpu.make_async_remote_copy(
                        src_ref=rest.at[0],
                        dst_ref=rest_in.at[pair, part],
                        send_sem=r_send.at[0],
                        recv_sem=r_recv.at[pair, part],
                        device_id={"x": xp},
                        device_id_type=MESH,
                    ).wait_recv()

            fr[pair, 0, OWN - REST : OWN] += rest_in[pair, 0] + rest_in[pair, 1]

    def deliver(pair):
        for way in range(2):
            yc[pair, way, 2].wait_recv()
            yc[pair, way, 3].wait_recv()
        done = total[pair, y] + (yr[pair, 0, 2] + yr[pair, 1, 2]) + (yr[pair, 0, 3] + yr[pair, 1, 3])
        for part in range(2):
            if part:
                fs[pair, 1, 0 : LEAD - OWN] = done[OWN:LEAD]
                fs[pair, 1, LEAD - OWN : OWN] = jnp.zeros((REST, WIDTH), F32)
            else:
                fs[pair, 0, 0:OWN] = done[0:OWN]
            fs[pair, part, OWN:PART] = done[LEAD:ROWS]
            same = at_home & (zl == part)

            @pl.when(same)
            def _():
                fr[pair, zl] = fs[pair, part]

            @pl.when(jnp.logical_not(same))
            def _():
                final_copy(pair, part).start()

    def final_copy(pair, part):
        return pltpu.make_async_remote_copy(
            src_ref=fs.at[pair, part],
            dst_ref=fr.at[pair, zl],
            send_sem=f_send.at[pair, part],
            recv_sem=f_recv.at[pair, zl],
            device_id={"y": owner_y, "zl": part, "zh": owner_h, "core": half},
            device_id_type=MESH,
        )

    def receive(pair):
        for part in range(2):

            @pl.when(jnp.logical_not(at_home & (zl == part)))
            def _():
                pltpu.make_async_remote_copy(
                    src_ref=fs.at[pair, part],
                    dst_ref=fr.at[pair, part],
                    send_sem=f_send.at[pair, part],
                    recv_sem=f_recv.at[pair, part],
                    device_id={"y": owner_y, "zl": part, "zh": owner_h, "core": half},
                    device_id_type=MESH,
                ).wait_recv()

        rest_receive(pair)
        both = fr[pair, 0] + fr[pair, 1]
        count = both[OWN + 4 : OWN + 5, 0:1]
        lane = lax.broadcasted_iota(jnp.int32, (OWN, WIDTH), 1)
        row = lax.broadcasted_iota(jnp.int32, (OWN, WIDTH), 0)
        own = lane == row + (x * BLOCK + zl * OWN)

        def column(line):
            return jnp.sum(jnp.where(own, line, 0.0), axis=1, keepdims=True)

        mean_first = both[OWN : OWN + 1] / count
        square_first = both[OWN + 1 : OWN + 2] / count
        mean_second = column(both[OWN + 2 : OWN + 3]) / count
        square_second = column(both[OWN + 3 : OWN + 4]) / count
        spread_first = jnp.sqrt(square_first - mean_first * mean_first + EPS)
        spread_second = jnp.sqrt(square_second - mean_second * mean_second + EPS)
        out_ref[pair] = (both[0:OWN] / count - mean_second * mean_first) / (spread_second * spread_first)

    def enter():
        owners = 4 * at_hub.astype(jnp.int32) - rest_home.astype(jnp.int32)
        pl.semaphore_wait(barrier, 12 - at_home.astype(jnp.int32) + owners)

    for load in loads:
        load.wait()
    pick_first(0)
    enter()
    offer(0, "a")
    offer(0, "p")
    pick_second(0)
    offer(0, "b")
    offer(0, "s")
    arrive(0, "p")
    multiply(0, 0, 0)
    pick_first(1)
    offer(1, "a")
    offer(1, "p")
    pick_second(1)
    offer(1, "b")
    offer(1, "s")
    pass_on(0, 0, 0)
    arrive(1, "p")
    multiply(1, 0, 0)
    w_step(0, 0)
    collect(0, 0, 0)
    pass_on(1, 0, 0)
    forward(0)
    w_step(0, 1)
    arrive(0, "ap")
    multiply(0, 0, 1)
    arrive(0, "b", "s")
    multiply(0, 1, 1)
    collect(1, 0, 0)
    multiply(0, 1, 0)
    w_step(1, 0)
    pass_on(0, 0, 1)
    w_gather(0)
    pass_on(0, 1, 1)
    forward(1)
    pass_on(0, 1, 0)
    w_step(1, 1)
    arrive(1, "ap")
    multiply(1, 0, 1)
    arrive(1, "b", "s")
    multiply(1, 1, 0)
    multiply(1, 1, 1)
    w_deliver(0)
    collect(0, 0, 1)
    w_step(2, 0)
    collect(0, 1, 1)
    collect(0, 1, 0)
    y_step(0, 0)
    pass_on(1, 0, 1)
    w_gather(1)
    pass_on(1, 1, 0)
    pass_on(1, 1, 1)
    w_step(2, 1)
    collect(1, 0, 1)
    y_step(0, 1)
    w_deliver(1)
    collect(1, 1, 0)
    collect(1, 1, 1)
    y_step(1, 0)
    w_gather(2)
    deliver(0)
    y_step(1, 1)
    w_deliver(2)
    receive(0)
    deliver(1)
    receive(1)

    for copy in sent:
        copy.wait_send()
    for pair in range(PAIRS):
        for part in range(2):

            @pl.when(jnp.logical_not(at_home & (zl == part)))
            def _():
                final_copy(pair, part).wait_send()
    for group, blocks in enumerate(GROUPS):

        @pl.when(jnp.logical_not(at_hub))
        def _():
            gather_copy(group, x).wait_send()

        for pair, jb, ih in blocks:

            @pl.when(at_hub & jnp.logical_not(rest_home & (src_jb == jb) & (ih == 0)))
            def _():
                rest_copy(pair, jb, ih).wait_send()


def cross(pair_table, image, view, embeddings):
    blocks = 4 * PAIRS
    dma = pltpu.SemaphoreType.DMA
    vmem = pl.BlockSpec(memory_space=pltpu.VMEM)
    return pl.pallas_call(
        cross_kernel,
        out_shape=jax.ShapeDtypeStruct((PAIRS, OWN, WIDTH), F32),
        in_specs=[pl.BlockSpec(memory_space=pltpu.SMEM), vmem, vmem, pl.BlockSpec(memory_space=pl.ANY)],
        out_specs=vmem,
        scratch_shapes=[
            pltpu.VMEM((STEPS * SLOTS, WIDTH), BF16),
            pltpu.VMEM((IMG_DEV, WIDTH), F32),
            pltpu.VMEM((IMG_DEV, 128), F32),
            pltpu.VMEM((PAIRS, 1, WIDTH), F32),
            pltpu.VMEM((PAIRS, IMG_DEV, WIDTH), BF16),
            pltpu.VMEM((PAIRS, WIDTH, IMG_DEV), BF16),
            pltpu.VMEM((PAIRS, STAT, WIDTH), F32),
            pltpu.VMEM((PAIRS, IMG_DEV, WIDTH), BF16),
            pltpu.VMEM((PAIRS, IMG_DEV, WIDTH), BF16),
            pltpu.VMEM((PAIRS, IMG_DEV, WIDTH), BF16),
            pltpu.VMEM((PAIRS, WIDTH, IMG_DEV), BF16),
            pltpu.VMEM((PAIRS, STAT, WIDTH), F32),
            pltpu.VMEM((PAIRS, 2, 2, STAT, WIDTH), F32),
            pltpu.VMEM((blocks, NX, 2, ROWS, WIDTH), F32),
            pltpu.VMEM((blocks, ROWS, WIDTH), F32),
            pltpu.VMEM((blocks, ROWS, WIDTH), F32),
            pltpu.VMEM((blocks, 2, ROWS, WIDTH), F32),
            pltpu.VMEM((blocks, 2, ROWS, WIDTH), F32),
            pltpu.VMEM((PAIRS, NY, ROWS, WIDTH), F32),
            pltpu.VMEM((PAIRS, 2, 4, ROWS, WIDTH), F32),
            pltpu.VMEM((PAIRS, 2, PART, WIDTH), F32),
            pltpu.VMEM((PAIRS, 2, PART, WIDTH), F32),
            *(pltpu.VMEM((NY, len(blocks_of), REST, WIDTH), F32) for blocks_of in GROUPS),
            *(pltpu.VMEM((2, 4, len(blocks_of), REST, WIDTH), F32) for blocks_of in GROUPS),
            pltpu.VMEM((blocks, REST, WIDTH), F32),
            pltpu.VMEM((PAIRS, 2, REST, WIDTH), F32),
            *(pltpu.VMEM((len(blocks_of), REST, WIDTH), F32) for blocks_of in GROUPS),
            *(pltpu.VMEM((NX, len(blocks_of), REST, WIDTH), F32) for blocks_of in GROUPS),
            dma((STEPS,)),
            dma((PAIRS, 5)),
            dma((PAIRS, 5)),
            dma((blocks, 6)),
            dma((blocks, 6)),
            dma((PAIRS, 2, 4)),
            dma((PAIRS, 2, 4)),
            dma((PAIRS, 2)),
            dma((PAIRS, 2)),
            dma((len(GROUPS), 2, 4)),
            dma((len(GROUPS), 2, 4)),
            dma((blocks,)),
            dma((PAIRS, 2)),
            dma((len(GROUPS),)),
            dma((len(GROUPS), NX)),
        ],
        compiler_params=pltpu.CompilerParams(collective_id=0, has_side_effects=True),
        name="cross",
    )(pair_table, image, view, embeddings)


def local(embeddings, slot_image, slot_view, pair_table):
    shape = (STEPS * TILE, 128)
    block = cross(pair_table, slot_image.reshape(shape), slot_view.reshape(shape), embeddings)
    return jnp.swapaxes(block, 1, 2)


def solution(mesh):
    split = Mesh(mesh.devices.reshape(NY, NX, 2, 4, 2), AXES)
    placed = (P(DP, FEAT), P(DP), P(DP), P())
    return jax.shard_map(local, mesh=split, in_specs=placed, out_specs=P(None, FEAT, DP), check_vma=False)
```

```python
import jax
import jax.numpy as jnp
from jax import lax
from jax.experimental import pallas as pl
from jax.experimental.pallas import tpu as pltpu
from jax.sharding import Mesh
from jax.sharding import PartitionSpec as P

WIN = 2048
IMG_DEV = 512
PAIRS = 2
WIDTH = 256
OWN = 32
NX, NY = 4, 8
BLOCK = 64
STAT = 8
LEAD = 48
REST = BLOCK - LEAD
ROWS = LEAD + STAT
PART = OWN + STAT
SENT = (PART, STAT + LEAD - OWN)
CUT = 32
REST_CUT = 8
GROUPS = (
    ((0, 0, 0), (1, 0, 0)),
    ((0, 1, 0), (0, 0, 1), (0, 1, 1)),
    ((1, 1, 0), (1, 0, 1), (1, 1, 1)),
)
SLOTS = 1024
STEPS = 5
TILE = SLOTS // 128
VIEW_STRIDE = 16
AXES = ("y", "x", "zl", "zh", "core")
FEAT = ("zh", "core")
DP = ("y", "x", "zl")
EPS = 1e-05
F32 = jnp.float32
BF16 = jnp.bfloat16
MESH = pl.DeviceIdType.MESH


def place_of(plane, core, jb, ih, half):
    ahead = (1 - jb) * (ih * half + (1 - ih) * (7 - 5 * half)) + jb * (4 + 2 * ih - half)
    return (2 * plane + core + NY + (1 - 2 * (plane % 2)) * ahead) % NY


def cross_kernel(
    pair_ref, image_ref, view_ref, emb_ref, out_ref,
    emb, acc, found, counts, x1_ref, x2_ref, stat_ref,
    x1p, x1a, x1ap, x2b, statb, x1stat, cb, relay_p, relay_m, from_m, from_p, total, yr, fs, fr,
    w0, w1, w2, v0, v1, v2, rest, rest_in, u0, u1, u2, g0, g1, g2,
    emb_sem, z_send, z_recv, x_send, x_recv, y_send, y_recv, f_send, f_recv, w_send, w_recv, r_send, r_recv, g_send, g_recv,
):
    y, x, zl, h, core = [lax.axis_index(axis) for axis in AXES]
    plane_a = h + 1 - 2 * (h % 2)
    plane_b = 3 - h
    other = 1 - core
    xp, xa, xm = (x + 1) % NX, (x + 2) % NX, (x + 3) % NX
    yp, ym = (y + 1) % NY, (y + NY - 1) % NY
    yp2, ym2 = (y + 2) % NY, (y + NY - 2) % NY

    mine = (2 * NY + (1 - 2 * (h % 2)) * (y - 2 * h - core)) % NY
    jb = ((mine + 1) // 4) % 2
    ih = ((mine < 2) | ((mine > 4) & (mine < 7))).astype(jnp.int32)
    half = (((mine > 0) & (mine < 4)) | (mine == 5)).astype(jnp.int32)
    owner_y = 2 * (h + jb * (3 - 2 * h)) + core
    owner_h = h + ih * (1 - 2 * (h % 2))
    at_home = (owner_y == y) & (owner_h == h) & (half == core)
    jh, src_core = y // 2, y % 2
    src_jb = (jh // 2 + h // 2) % 2
    src_h = jh + src_jb * (3 - 2 * jh)
    src_ih = (src_h + h) % 2
    src_y = place_of(src_h, src_core, src_jb, src_ih, core)
    rest_y = 2 * x + core
    rest_home = (rest_y == y) & (src_h == h) & (zl == 1)
    hub = y // 2
    at_hub = x == hub

    loads = []
    for step in range(STEPS):
        rows = slice(step * SLOTS, (step + 1) * SLOTS)
        loads.append(pltpu.make_async_copy(emb_ref.at[rows], emb.at[rows], emb_sem.at[step]))
        loads[-1].start()

    barrier = pltpu.get_barrier_semaphore()
    for peer in ({"x": xp}, {"x": xm}, {"x": xa}, {"y": yp}, {"y": ym}, {"y": yp2}, {"y": ym2}, {"zh": plane_a}, {"zh": plane_b}, {"core": other}):
        pl.semaphore_signal(barrier, inc=1, device_id=peer, device_id_type=MESH)
    for part in range(2):

        @pl.when(jnp.logical_not(at_home & (zl == part)))
        def _():
            pl.semaphore_signal(
                barrier,
                inc=1,
                device_id={"y": src_y, "zl": part, "zh": src_h, "core": src_core},
                device_id_type=MESH,
            )

    for part in range(2):

        @pl.when((zl == 1) & jnp.logical_not(rest_home & (zl == part)))
        def _():
            pl.semaphore_signal(
                barrier,
                inc=1,
                device_id={"y": rest_y, "zl": part, "zh": src_h, "core": src_core},
                device_id_type=MESH,
            )

    sent = []

    def send(src, dst, send_sem, recv_sem, peer):
        copy = pltpu.make_async_remote_copy(
            src_ref=src, dst_ref=dst, send_sem=send_sem, recv_sem=recv_sem, device_id=peer, device_id_type=MESH
        )
        copy.start()
        sent.append(copy)
        return copy

    z = {}

    def offer(pair, name):
        slot, src, dst, peer = {
            "p": (0, x1_ref, x1p, {"core": other}),
            "b": (1, x2_ref, x2b, {"zh": plane_b}),
            "s": (2, stat_ref, statb, {"zh": plane_b}),
            "a": (3, x1_ref, x1a, {"zh": plane_a}),
        }[name]
        z[name, pair] = send(src.at[pair], dst.at[pair], z_send.at[pair, slot], z_recv.at[pair, slot], peer)

    def arrive(pair, *names):
        for name in names:
            z[name, pair].wait_recv()

    base = (y * NX * 2 + x * 2 + zl) * IMG_DEV
    wanted = (lax.broadcasted_iota(jnp.int32, (IMG_DEV, 128), 0) + base) * VIEW_STRIDE

    def pick(pair, side):
        target = wanted + pair_ref[pair, side]
        second = wanted + pair_ref[pair, 1]
        acc[...] = jnp.zeros_like(acc)
        if side == 0:
            found[...] = jnp.zeros_like(found)

        def step(index, carry):
            key = image_ref[pl.ds(pl.multiple_of(index * TILE, TILE), TILE), :] * VIEW_STRIDE
            key += view_ref[pl.ds(pl.multiple_of(index * TILE, TILE), TILE), :]
            keys = [key[row : row + 1, :] for row in range(TILE)]
            chosen = jnp.concatenate([jnp.where(one == target, 1.0, 0.0).astype(BF16) for one in keys], axis=1)
            rows = emb[pl.ds(pl.multiple_of(index * SLOTS, SLOTS), SLOTS), :]
            acc[...] += jnp.dot(chosen, rows, preferred_element_type=F32)
            if side == 0:
                hits = [jnp.where(one == second, 1.0, 0.0) for one in keys]
                found[...] += sum(hits[1:], hits[0])
            return carry

        lax.fori_loop(0, STEPS, step, 0)

    def pick_first(pair):
        pick(pair, 0)
        present = jnp.sum(found[...], axis=1, keepdims=True)
        x1_ref[pair] = jnp.where(present > 0.5, acc[...], 0.0).astype(BF16)
        counts[pair] = jnp.broadcast_to(jnp.sum(present, axis=0, keepdims=True), (1, WIDTH))

    def pick_second(pair):
        pick(pair, 1)
        row = lax.broadcasted_iota(jnp.int32, (STAT, WIDTH), 0)
        rows = acc[...]
        x2_ref[pair] = rows.T.astype(BF16)
        plain = jnp.sum(rows, axis=0, keepdims=True)
        square = jnp.sum(rows * rows, axis=0, keepdims=True)
        stat_ref[pair] = jnp.where(
            row == 2, plain, jnp.where(row == 3, square, jnp.where(row == 4, counts[pair], 0.0))
        )

    def forward(pair):
        arrive(pair, "a")
        z["ap", pair] = send(
            x1a.at[pair], x1ap.at[pair], z_send.at[pair, 4], z_recv.at[pair, 4], {"core": other}
        )

    stats_done = set()
    xc = {}

    def block_of(pair, jb, ih):
        return 4 * pair + 2 * jb + ih

    def multiply(pair, jb, ih):
        k = block_of(pair, jb, ih)
        group, place = next(
            (g, blocks.index((pair, jb, ih))) for g, blocks in enumerate(GROUPS) if (pair, jb, ih) in blocks
        )
        second = (x2b if jb else x2_ref)[pair]
        stat = (statb if jb else stat_ref)[pair]
        row = lax.broadcasted_iota(jnp.int32, (STAT, WIDTH), 0)
        for slot, (ref, half) in enumerate((((x1a if ih else x1_ref), core), ((x1ap if ih else x1p), other))):
            first = ref[pair]
            if (pair, ih, slot) not in stats_done:
                stats_done.add((pair, ih, slot))
                wide = first.astype(F32)
                plain = jnp.sum(wide, axis=0, keepdims=True)
                square = jnp.sum(wide * wide, axis=0, keepdims=True)
                x1stat[pair, ih, slot] = jnp.where(row == 0, plain, jnp.where(row == 1, square, 0.0))
            product = jnp.dot(second, first, preferred_element_type=F32)
            sums = x1stat[pair, ih, slot] + stat
            for dest in range(NX):
                cb[k, dest, half, 0:LEAD] = product[dest * BLOCK : dest * BLOCK + LEAD]
                cb[k, dest, half, LEAD:ROWS] = sums
                w[group][2 * dest + half, place] = product[dest * BLOCK + LEAD : (dest + 1) * BLOCK]
        for slot, (src, dst, to) in enumerate(
            (
                (cb.at[k, xa, 0], relay_p.at[k], xp),
                (cb.at[k, xa, 1], relay_m.at[k], xm),
                (cb.at[k, xp, 1], from_m.at[k, 1], xp),
                (cb.at[k, xm, 0], from_p.at[k, 0], xm),
            )
        ):
            xc[k, slot] = send(src, dst, x_send.at[k, slot], x_recv.at[k, slot], {"x": to})

    def pass_on(pair, jb, ih):
        k = block_of(pair, jb, ih)
        xc[k, 0].wait_recv()
        cb[k, xp, 0] += relay_p[k]
        xc[k, 4] = send(cb.at[k, xp, 0], from_m.at[k, 0], x_send.at[k, 4], x_recv.at[k, 4], {"x": xp})
        xc[k, 1].wait_recv()
        cb[k, xm, 1] += relay_m[k]
        xc[k, 5] = send(cb.at[k, xm, 1], from_p.at[k, 1], x_send.at[k, 5], x_recv.at[k, 5], {"x": xm})

    def collect(pair, jb, ih):
        k = block_of(pair, jb, ih)
        for slot in (2, 3, 4, 5):
            xc[k, slot].wait_recv()
        for half in range(2):
            total[pair, place_of(h, core, jb, ih, half)] = cb[k, x, half] + from_m[k, half] + from_p[k, half]

    def y_ways(key, copies, part, landing, send_sem, recv_sem, cut, step):
        for way in range(2):
            one, two = (ym, ym2) if way else (yp, yp2)
            rows = slice(cut, None) if way else slice(0, cut)

            def at(distance):
                return (y + (NY - distance if way else distance)) % NY

            def go(slot, src, dst, to):
                copies[key, way, slot] = send(src, dst, send_sem(way, slot), recv_sem(way, slot), {"y": to})

            if step == 0:
                far = part(at(4), rows)
                go(0, far, landing(way, 0, slice(0, far.shape[-2])), two)
                go(1, part(at(3)), landing(way, 1), one)
                go(2, part(at(1)), landing(way, 2), one)
                continue
            copies[key, way, 0].wait_recv()
            copies[key, way, 1].wait_recv()
            second = part(at(2))
            second[...] += landing(way, 1)[...]
            half_of = part(at(2), rows)
            half_of[...] += landing(way, 0, slice(0, half_of.shape[-2]))[...]
            go(3, second, landing(way, 3), two)

    yc = {}

    def y_step(pair, step):
        y_ways(
            pair,
            yc,
            lambda place, rows=slice(0, ROWS): total.at[pair, place, slice(rows.start, rows.stop or ROWS)],
            lambda way, slot, rows=slice(0, ROWS): yr.at[pair, way, slot, rows],
            lambda way, slot: y_send.at[pair, way, slot],
            lambda way, slot: y_recv.at[pair, way, slot],
            CUT,
            step,
        )

    w, v = (w0, w1, w2), (v0, v1, v2)
    wc = {}

    def w_step(group, step):
        y_ways(
            group,
            wc,
            lambda place, rows=slice(0, REST): w[group].at[place, :, slice(rows.start, rows.stop or REST)],
            lambda way, slot, rows=slice(0, REST): v[group].at[way, slot, :, rows],
            lambda way, slot: w_send.at[group, way, slot],
            lambda way, slot: w_recv.at[group, way, slot],
            REST_CUT,
            step,
        )

    def rest_copy(pair, jb, ih):
        k = block_of(pair, jb, ih)
        return pltpu.make_async_remote_copy(
            src_ref=rest.at[k],
            dst_ref=rest_in.at[pair, zl],
            send_sem=r_send.at[k],
            recv_sem=r_recv.at[pair, zl],
            device_id={
                "y": 2 * (plane_b if jb else h) + core,
                "x": hub,
                "zl": 1,
                "zh": plane_a if ih else h,
                "core": y % 2,
            },
            device_id_type=MESH,
        )

    u, gx = (u0, u1, u2), (g0, g1, g2)

    def gather_copy(group, from_x, to=hub):
        return pltpu.make_async_remote_copy(
            src_ref=u[group],
            dst_ref=gx[group].at[from_x],
            send_sem=g_send.at[group],
            recv_sem=g_recv.at[group, from_x],
            device_id={"x": to},
            device_id_type=MESH,
        )

    def w_gather(group):
        for way in range(2):
            wc[group, way, 2].wait_recv()
            wc[group, way, 3].wait_recv()
        near = v[group][0, 2] + v[group][1, 2]
        u[group][...] = w[group][y] + near + (v[group][0, 3] + v[group][1, 3])

        @pl.when(jnp.logical_not(at_hub))
        def _():
            gather_copy(group, x).start()

    def w_deliver(group):
        @pl.when(at_hub)
        def _():
            for from_x in range(NX):

                @pl.when(x != from_x)
                def _():
                    gather_copy(group, from_x, xp).wait_recv()

            summed = u[group][...] + gx[group][xa] + (gx[group][xp] + gx[group][xm])
            for place, (pair, jb, ih) in enumerate(GROUPS[group]):
                rest[block_of(pair, jb, ih)] = summed[place]
            for pair, jb, ih in GROUPS[group]:
                if ih:
                    rest_copy(pair, jb, ih).start()
                    continue
                same = rest_home & (src_jb == jb)

                @pl.when(same)
                def _():
                    rest_in[pair, zl] = rest[block_of(pair, jb, ih)]

                @pl.when(jnp.logical_not(same))
                def _():
                    rest_copy(pair, jb, ih).start()

    def rest_receive(pair):
        @pl.when(zl == 1)
        def _():
            for part in range(2):

                @pl.when(jnp.logical_not(rest_home & (zl == part)))
                def _():
                    pltpu.make_async_remote_copy(
                        src_ref=rest.at[0],
                        dst_ref=rest_in.at[pair, part],
                        send_sem=r_send.at[0],
                        recv_sem=r_recv.at[pair, part],
                        device_id={"x": xp},
                        device_id_type=MESH,
                    ).wait_recv()

            fr[pair, 0, SENT[1] : PART] = rest_in[pair, 0] + rest_in[pair, 1]
            fr[pair, 1, SENT[1] : PART] = jnp.zeros((REST, WIDTH), F32)

    def deliver(pair):
        for way in range(2):
            yc[pair, way, 2].wait_recv()
            yc[pair, way, 3].wait_recv()
        done = total[pair, y] + (yr[pair, 0, 2] + yr[pair, 1, 2]) + (yr[pair, 0, 3] + yr[pair, 1, 3])
        for part in range(2):
            fs[pair, part, 0:STAT] = done[LEAD:ROWS]
            fs[pair, part, STAT : SENT[part]] = done[OWN:LEAD] if part else done[0:OWN]
            same = at_home & (zl == part)

            @pl.when(same)
            def _():
                fr[pair, zl, 0 : SENT[part]] = fs[pair, part, 0 : SENT[part]]

            @pl.when(jnp.logical_not(same))
            def _():
                final_copy(pair, part).start()

    def final_copy(pair, part):
        return pltpu.make_async_remote_copy(
            src_ref=fs.at[pair, part, 0 : SENT[part]],
            dst_ref=fr.at[pair, zl, 0 : SENT[part]],
            send_sem=f_send.at[pair, part],
            recv_sem=f_recv.at[pair, zl],
            device_id={"y": owner_y, "zl": part, "zh": owner_h, "core": half},
            device_id_type=MESH,
        )

    def receive(pair):
        for part in range(2):

            for own in range(2):

                @pl.when((zl == own) & jnp.logical_not(at_home & (zl == part)))
                def _():
                    pltpu.make_async_remote_copy(
                        src_ref=fs.at[pair, part, 0 : SENT[own]],
                        dst_ref=fr.at[pair, part, 0 : SENT[own]],
                        send_sem=f_send.at[pair, part],
                        recv_sem=f_recv.at[pair, part],
                        device_id={"x": xp},
                        device_id_type=MESH,
                    ).wait_recv()

        rest_receive(pair)
        both = fr[pair, 0] + fr[pair, 1]
        count = both[4 : 5, 0:1]
        lane = lax.broadcasted_iota(jnp.int32, (OWN, WIDTH), 1)
        row = lax.broadcasted_iota(jnp.int32, (OWN, WIDTH), 0)
        own = lane == row + (x * BLOCK + zl * OWN)

        def column(line):
            return jnp.sum(jnp.where(own, line, 0.0), axis=1, keepdims=True)

        mean_first = both[0:1] / count
        square_first = both[1 : 2] / count
        mean_second = column(both[2 : 3]) / count
        square_second = column(both[3 : 4]) / count
        spread_first = jnp.sqrt(square_first - mean_first * mean_first + EPS)
        spread_second = jnp.sqrt(square_second - mean_second * mean_second + EPS)
        out_ref[pair] = (both[STAT:PART] / count - mean_second * mean_first) / (spread_second * spread_first)

    def enter():
        owners = 4 * at_hub.astype(jnp.int32) - rest_home.astype(jnp.int32)
        pl.semaphore_wait(barrier, 12 - at_home.astype(jnp.int32) + owners)

    for load in loads:
        load.wait()
    pick_first(0)
    enter()
    offer(0, "a")
    offer(0, "p")
    pick_second(0)
    offer(0, "b")
    offer(0, "s")
    arrive(0, "p")
    multiply(0, 0, 0)
    pick_first(1)
    offer(1, "a")
    offer(1, "p")
    pick_second(1)
    offer(1, "b")
    offer(1, "s")
    pass_on(0, 0, 0)
    arrive(1, "p")
    multiply(1, 0, 0)
    w_step(0, 0)
    collect(0, 0, 0)
    pass_on(1, 0, 0)
    forward(0)
    w_step(0, 1)
    arrive(0, "ap")
    multiply(0, 0, 1)
    arrive(0, "b", "s")
    multiply(0, 1, 1)
    collect(1, 0, 0)
    multiply(0, 1, 0)
    w_step(1, 0)
    pass_on(0, 0, 1)
    w_gather(0)
    pass_on(0, 1, 1)
    forward(1)
    pass_on(0, 1, 0)
    w_step(1, 1)
    arrive(1, "ap")
    multiply(1, 0, 1)
    arrive(1, "b", "s")
    multiply(1, 1, 0)
    multiply(1, 1, 1)
    w_deliver(0)
    collect(0, 0, 1)
    w_step(2, 0)
    collect(0, 1, 1)
    collect(0, 1, 0)
    y_step(0, 0)
    pass_on(1, 0, 1)
    w_gather(1)
    pass_on(1, 1, 0)
    pass_on(1, 1, 1)
    w_step(2, 1)
    collect(1, 0, 1)
    y_step(0, 1)
    w_deliver(1)
    collect(1, 1, 0)
    collect(1, 1, 1)
    y_step(1, 0)
    w_gather(2)
    deliver(0)
    y_step(1, 1)
    w_deliver(2)
    receive(0)
    deliver(1)
    receive(1)

    for copy in sent:
        copy.wait_send()
    for pair in range(PAIRS):
        for part in range(2):

            @pl.when(jnp.logical_not(at_home & (zl == part)))
            def _():
                final_copy(pair, part).wait_send()
    for group, blocks in enumerate(GROUPS):

        @pl.when(jnp.logical_not(at_hub))
        def _():
            gather_copy(group, x).wait_send()

        for pair, jb, ih in blocks:

            @pl.when(at_hub & jnp.logical_not(rest_home & (src_jb == jb) & (ih == 0)))
            def _():
                rest_copy(pair, jb, ih).wait_send()


def cross(pair_table, image, view, embeddings):
    blocks = 4 * PAIRS
    dma = pltpu.SemaphoreType.DMA
    vmem = pl.BlockSpec(memory_space=pltpu.VMEM)
    return pl.pallas_call(
        cross_kernel,
        out_shape=jax.ShapeDtypeStruct((PAIRS, OWN, WIDTH), F32),
        in_specs=[pl.BlockSpec(memory_space=pltpu.SMEM), vmem, vmem, pl.BlockSpec(memory_space=pl.ANY)],
        out_specs=vmem,
        scratch_shapes=[
            pltpu.VMEM((STEPS * SLOTS, WIDTH), BF16),
            pltpu.VMEM((IMG_DEV, WIDTH), F32),
            pltpu.VMEM((IMG_DEV, 128), F32),
            pltpu.VMEM((PAIRS, 1, WIDTH), F32),
            pltpu.VMEM((PAIRS, IMG_DEV, WIDTH), BF16),
            pltpu.VMEM((PAIRS, WIDTH, IMG_DEV), BF16),
            pltpu.VMEM((PAIRS, STAT, WIDTH), F32),
            pltpu.VMEM((PAIRS, IMG_DEV, WIDTH), BF16),
            pltpu.VMEM((PAIRS, IMG_DEV, WIDTH), BF16),
            pltpu.VMEM((PAIRS, IMG_DEV, WIDTH), BF16),
            pltpu.VMEM((PAIRS, WIDTH, IMG_DEV), BF16),
            pltpu.VMEM((PAIRS, STAT, WIDTH), F32),
            pltpu.VMEM((PAIRS, 2, 2, STAT, WIDTH), F32),
            pltpu.VMEM((blocks, NX, 2, ROWS, WIDTH), F32),
            pltpu.VMEM((blocks, ROWS, WIDTH), F32),
            pltpu.VMEM((blocks, ROWS, WIDTH), F32),
            pltpu.VMEM((blocks, 2, ROWS, WIDTH), F32),
            pltpu.VMEM((blocks, 2, ROWS, WIDTH), F32),
            pltpu.VMEM((PAIRS, NY, ROWS, WIDTH), F32),
            pltpu.VMEM((PAIRS, 2, 4, ROWS, WIDTH), F32),
            pltpu.VMEM((PAIRS, 2, PART, WIDTH), F32),
            pltpu.VMEM((PAIRS, 2, PART, WIDTH), F32),
            *(pltpu.VMEM((NY, len(blocks_of), REST, WIDTH), F32) for blocks_of in GROUPS),
            *(pltpu.VMEM((2, 4, len(blocks_of), REST, WIDTH), F32) for blocks_of in GROUPS),
            pltpu.VMEM((blocks, REST, WIDTH), F32),
            pltpu.VMEM((PAIRS, 2, REST, WIDTH), F32),
            *(pltpu.VMEM((len(blocks_of), REST, WIDTH), F32) for blocks_of in GROUPS),
            *(pltpu.VMEM((NX, len(blocks_of), REST, WIDTH), F32) for blocks_of in GROUPS),
            dma((STEPS,)),
            dma((PAIRS, 5)),
            dma((PAIRS, 5)),
            dma((blocks, 6)),
            dma((blocks, 6)),
            dma((PAIRS, 2, 4)),
            dma((PAIRS, 2, 4)),
            dma((PAIRS, 2)),
            dma((PAIRS, 2)),
            dma((len(GROUPS), 2, 4)),
            dma((len(GROUPS), 2, 4)),
            dma((blocks,)),
            dma((PAIRS, 2)),
            dma((len(GROUPS),)),
            dma((len(GROUPS), NX)),
        ],
        compiler_params=pltpu.CompilerParams(collective_id=0, has_side_effects=True),
        name="cross",
    )(pair_table, image, view, embeddings)


def local(embeddings, slot_image, slot_view, pair_table):
    shape = (STEPS * TILE, 128)
    block = cross(pair_table, slot_image.reshape(shape), slot_view.reshape(shape), embeddings)
    return jnp.swapaxes(block, 1, 2)


def solution(mesh):
    split = Mesh(mesh.devices.reshape(NY, NX, 2, 4, 2), AXES)
    placed = (P(DP, FEAT), P(DP), P(DP), P())
    return jax.shard_map(local, mesh=split, in_specs=placed, out_specs=P(None, FEAT, DP), check_vma=False)
```

```python
import jax
import jax.numpy as jnp
from jax import lax
from jax.experimental import pallas as pl
from jax.experimental.pallas import tpu as pltpu
from jax.sharding import Mesh
from jax.sharding import PartitionSpec as P

WIN = 2048
IMG_DEV = 512
PAIRS = 2
WIDTH = 256
OWN = 32
NX, NY = 4, 8
BLOCK = 64
STAT = 8
LEAD = 48
REST = BLOCK - LEAD
ROWS = LEAD + STAT
PART = OWN + STAT
SENT = (PART, STAT + LEAD - OWN)
CUT = 32
REST_CUT = 8
GROUPS = (
    ((0, 0, 0), (1, 0, 0)),
    ((0, 1, 0), (0, 0, 1), (0, 1, 1)),
    ((1, 1, 0), (1, 0, 1), (1, 1, 1)),
)
SLOTS = 1024
STEPS = 5
TILE = SLOTS // 128
VIEW_STRIDE = 16
AXES = ("y", "x", "zl", "zh", "core")
FEAT = ("zh", "core")
DP = ("y", "x", "zl")
EPS = 1e-05
F32 = jnp.float32
BF16 = jnp.bfloat16
MESH = pl.DeviceIdType.MESH


def place_of(plane, core, jb, ih, half):
    ahead = (1 - jb) * (ih * half + (1 - ih) * (7 - 5 * half)) + jb * (4 + 2 * ih - half)
    return (2 * plane + core + NY + (1 - 2 * (plane % 2)) * ahead) % NY


def cross_kernel(
    pair_ref, image_ref, view_ref, emb_ref, out_ref,
    emb, acc, found, counts, x1_ref, x2_ref, stat_ref,
    x1p, x1a, x1ap, x2b, statb, x1stat, cb, relay_p, relay_m, from_m, from_p, total, yr, fs, fr,
    w0, w1, w2, v0, v1, v2, rest, rest_in, u0, u1, u2, g0, g1, g2,
    emb_sem, z_send, z_recv, x_send, x_recv, y_send, y_recv, f_send, f_recv, w_send, w_recv, r_send, r_recv, g_send, g_recv,
):
    y, x, zl, h, core = [lax.axis_index(axis) for axis in AXES]
    plane_a = h + 1 - 2 * (h % 2)
    plane_b = 3 - h
    other = 1 - core
    xp, xa, xm = (x + 1) % NX, (x + 2) % NX, (x + 3) % NX
    yp, ym = (y + 1) % NY, (y + NY - 1) % NY
    yp2, ym2 = (y + 2) % NY, (y + NY - 2) % NY

    mine = (2 * NY + (1 - 2 * (h % 2)) * (y - 2 * h - core)) % NY
    jb = ((mine + 1) // 4) % 2
    ih = ((mine < 2) | ((mine > 4) & (mine < 7))).astype(jnp.int32)
    half = (((mine > 0) & (mine < 4)) | (mine == 5)).astype(jnp.int32)
    owner_y = 2 * (h + jb * (3 - 2 * h)) + core
    owner_h = h + ih * (1 - 2 * (h % 2))
    at_home = (owner_y == y) & (owner_h == h) & (half == core)
    jh, src_core = y // 2, y % 2
    src_jb = (jh // 2 + h // 2) % 2
    src_h = jh + src_jb * (3 - 2 * jh)
    src_ih = (src_h + h) % 2
    src_y = place_of(src_h, src_core, src_jb, src_ih, core)
    rest_y = 2 * x + core
    rest_home = (rest_y == y) & (src_h == h) & (zl == 1)
    hub = y // 2
    at_hub = x == hub

    def load(step):
        rows = pl.ds(pl.multiple_of(step * SLOTS, SLOTS), SLOTS)
        return pltpu.make_async_copy(emb_ref.at[rows], emb.at[rows], emb_sem.at[step])

    for step in range(STEPS):
        load(step).start()

    barrier = pltpu.get_barrier_semaphore()
    for peer in ({"x": xp}, {"x": xm}, {"x": xa}, {"y": yp}, {"y": ym}, {"y": yp2}, {"y": ym2}, {"zh": plane_a}, {"zh": plane_b}, {"core": other}):
        pl.semaphore_signal(barrier, inc=1, device_id=peer, device_id_type=MESH)
    for part in range(2):

        @pl.when(jnp.logical_not(at_home & (zl == part)))
        def _():
            pl.semaphore_signal(
                barrier,
                inc=1,
                device_id={"y": src_y, "zl": part, "zh": src_h, "core": src_core},
                device_id_type=MESH,
            )

    for part in range(2):

        @pl.when((zl == 1) & jnp.logical_not(rest_home & (zl == part)))
        def _():
            pl.semaphore_signal(
                barrier,
                inc=1,
                device_id={"y": rest_y, "zl": part, "zh": src_h, "core": src_core},
                device_id_type=MESH,
            )

    sent = []

    def send(src, dst, send_sem, recv_sem, peer):
        copy = pltpu.make_async_remote_copy(
            src_ref=src, dst_ref=dst, send_sem=send_sem, recv_sem=recv_sem, device_id=peer, device_id_type=MESH
        )
        copy.start()
        sent.append(copy)
        return copy

    z = {}

    def offer(pair, name):
        slot, src, dst, peer = {
            "p": (0, x1_ref, x1p, {"core": other}),
            "b": (1, x2_ref, x2b, {"zh": plane_b}),
            "s": (2, stat_ref, statb, {"zh": plane_b}),
            "a": (3, x1_ref, x1a, {"zh": plane_a}),
        }[name]
        z[name, pair] = send(src.at[pair], dst.at[pair], z_send.at[pair, slot], z_recv.at[pair, slot], peer)

    def arrive(pair, *names):
        for name in names:
            z[name, pair].wait_recv()

    base = (y * NX * 2 + x * 2 + zl) * IMG_DEV
    wanted = (lax.broadcasted_iota(jnp.int32, (IMG_DEV, 128), 0) + base) * VIEW_STRIDE

    def pick(pair, side):
        target = wanted + pair_ref[pair, side]
        second = wanted + pair_ref[pair, 1]
        acc[...] = jnp.zeros_like(acc)
        if side == 0:
            found[...] = jnp.zeros_like(found)

        def step(index, carry):
            if (pair, side) == (0, 0):
                load(index).wait()
            key = image_ref[pl.ds(pl.multiple_of(index * TILE, TILE), TILE), :] * VIEW_STRIDE
            key += view_ref[pl.ds(pl.multiple_of(index * TILE, TILE), TILE), :]
            keys = [key[row : row + 1, :] for row in range(TILE)]
            chosen = jnp.concatenate([jnp.where(one == target, 1.0, 0.0).astype(BF16) for one in keys], axis=1)
            rows = emb[pl.ds(pl.multiple_of(index * SLOTS, SLOTS), SLOTS), :]
            acc[...] += jnp.dot(chosen, rows, preferred_element_type=F32)
            if side == 0:
                hits = [jnp.where(one == second, 1.0, 0.0) for one in keys]
                found[...] += sum(hits[1:], hits[0])
            return carry

        lax.fori_loop(0, STEPS, step, 0)

    def pick_first(pair):
        pick(pair, 0)
        present = jnp.sum(found[...], axis=1, keepdims=True)
        x1_ref[pair] = jnp.where(present > 0.5, acc[...], 0.0).astype(BF16)
        counts[pair] = jnp.broadcast_to(jnp.sum(present, axis=0, keepdims=True), (1, WIDTH))

    def pick_second(pair):
        pick(pair, 1)
        row = lax.broadcasted_iota(jnp.int32, (STAT, WIDTH), 0)
        rows = acc[...]
        x2_ref[pair] = rows.T.astype(BF16)
        plain = jnp.sum(rows, axis=0, keepdims=True)
        square = jnp.sum(rows * rows, axis=0, keepdims=True)
        stat_ref[pair] = jnp.where(
            row == 2, plain, jnp.where(row == 3, square, jnp.where(row == 4, counts[pair], 0.0))
        )

    def forward(pair):
        arrive(pair, "a")
        z["ap", pair] = send(
            x1a.at[pair], x1ap.at[pair], z_send.at[pair, 4], z_recv.at[pair, 4], {"core": other}
        )

    stats_done = set()
    xc = {}

    def block_of(pair, jb, ih):
        return 4 * pair + 2 * jb + ih

    def multiply(pair, jb, ih):
        k = block_of(pair, jb, ih)
        group, place = next(
            (g, blocks.index((pair, jb, ih))) for g, blocks in enumerate(GROUPS) if (pair, jb, ih) in blocks
        )
        second = (x2b if jb else x2_ref)[pair]
        stat = (statb if jb else stat_ref)[pair]
        row = lax.broadcasted_iota(jnp.int32, (STAT, WIDTH), 0)
        for slot, (ref, half) in enumerate((((x1a if ih else x1_ref), core), ((x1ap if ih else x1p), other))):
            first = ref[pair]
            if (pair, ih, slot) not in stats_done:
                stats_done.add((pair, ih, slot))
                wide = first.astype(F32)
                plain = jnp.sum(wide, axis=0, keepdims=True)
                square = jnp.sum(wide * wide, axis=0, keepdims=True)
                x1stat[pair, ih, slot] = jnp.where(row == 0, plain, jnp.where(row == 1, square, 0.0))
            product = jnp.dot(second, first, preferred_element_type=F32)
            sums = x1stat[pair, ih, slot] + stat
            for dest in range(NX):
                cb[k, dest, half, 0:LEAD] = product[dest * BLOCK : dest * BLOCK + LEAD]
                cb[k, dest, half, LEAD:ROWS] = sums
                w[group][2 * dest + half, place] = product[dest * BLOCK + LEAD : (dest + 1) * BLOCK]
        for slot, (src, dst, to) in enumerate(
            (
                (cb.at[k, xa, 0], relay_p.at[k], xp),
                (cb.at[k, xa, 1], relay_m.at[k], xm),
                (cb.at[k, xp, 1], from_m.at[k, 1], xp),
                (cb.at[k, xm, 0], from_p.at[k, 0], xm),
            )
        ):
            xc[k, slot] = send(src, dst, x_send.at[k, slot], x_recv.at[k, slot], {"x": to})

    def pass_on(pair, jb, ih):
        k = block_of(pair, jb, ih)
        xc[k, 0].wait_recv()
        cb[k, xp, 0] += relay_p[k]
        xc[k, 4] = send(cb.at[k, xp, 0], from_m.at[k, 0], x_send.at[k, 4], x_recv.at[k, 4], {"x": xp})
        xc[k, 1].wait_recv()
        cb[k, xm, 1] += relay_m[k]
        xc[k, 5] = send(cb.at[k, xm, 1], from_p.at[k, 1], x_send.at[k, 5], x_recv.at[k, 5], {"x": xm})

    def collect(pair, jb, ih):
        k = block_of(pair, jb, ih)
        for slot in (2, 3, 4, 5):
            xc[k, slot].wait_recv()
        for half in range(2):
            total[pair, place_of(h, core, jb, ih, half)] = cb[k, x, half] + from_m[k, half] + from_p[k, half]

    def y_ways(key, copies, part, landing, send_sem, recv_sem, cut, step):
        for way in range(2):
            one, two = (ym, ym2) if way else (yp, yp2)
            rows = slice(cut, None) if way else slice(0, cut)

            def at(distance):
                return (y + (NY - distance if way else distance)) % NY

            def go(slot, src, dst, to):
                copies[key, way, slot] = send(src, dst, send_sem(way, slot), recv_sem(way, slot), {"y": to})

            if step == 0:
                far = part(at(4), rows)
                go(0, far, landing(way, 0, slice(0, far.shape[-2])), two)
                go(1, part(at(3)), landing(way, 1), one)
                go(2, part(at(1)), landing(way, 2), one)
                continue
            copies[key, way, 0].wait_recv()
            copies[key, way, 1].wait_recv()
            second = part(at(2))
            second[...] += landing(way, 1)[...]
            half_of = part(at(2), rows)
            half_of[...] += landing(way, 0, slice(0, half_of.shape[-2]))[...]
            go(3, second, landing(way, 3), two)

    yc = {}

    def y_step(pair, step):
        y_ways(
            pair,
            yc,
            lambda place, rows=slice(0, ROWS): total.at[pair, place, slice(rows.start, rows.stop or ROWS)],
            lambda way, slot, rows=slice(0, ROWS): yr.at[pair, way, slot, rows],
            lambda way, slot: y_send.at[pair, way, slot],
            lambda way, slot: y_recv.at[pair, way, slot],
            CUT,
            step,
        )

    w, v = (w0, w1, w2), (v0, v1, v2)
    wc = {}

    def w_step(group, step):
        y_ways(
            group,
            wc,
            lambda place, rows=slice(0, REST): w[group].at[place, :, slice(rows.start, rows.stop or REST)],
            lambda way, slot, rows=slice(0, REST): v[group].at[way, slot, :, rows],
            lambda way, slot: w_send.at[group, way, slot],
            lambda way, slot: w_recv.at[group, way, slot],
            REST_CUT,
            step,
        )

    def rest_copy(pair, jb, ih):
        k = block_of(pair, jb, ih)
        return pltpu.make_async_remote_copy(
            src_ref=rest.at[k],
            dst_ref=rest_in.at[pair, zl],
            send_sem=r_send.at[k],
            recv_sem=r_recv.at[pair, zl],
            device_id={
                "y": 2 * (plane_b if jb else h) + core,
                "x": hub,
                "zl": 1,
                "zh": plane_a if ih else h,
                "core": y % 2,
            },
            device_id_type=MESH,
        )

    u, gx = (u0, u1, u2), (g0, g1, g2)

    def gather_copy(group, from_x, to=hub):
        return pltpu.make_async_remote_copy(
            src_ref=u[group],
            dst_ref=gx[group].at[from_x],
            send_sem=g_send.at[group],
            recv_sem=g_recv.at[group, from_x],
            device_id={"x": to},
            device_id_type=MESH,
        )

    def w_gather(group):
        for way in range(2):
            wc[group, way, 2].wait_recv()
            wc[group, way, 3].wait_recv()
        near = v[group][0, 2] + v[group][1, 2]
        u[group][...] = w[group][y] + near + (v[group][0, 3] + v[group][1, 3])

        @pl.when(jnp.logical_not(at_hub))
        def _():
            gather_copy(group, x).start()

    def w_deliver(group):
        @pl.when(at_hub)
        def _():
            for from_x in range(NX):

                @pl.when(x != from_x)
                def _():
                    gather_copy(group, from_x, xp).wait_recv()

            summed = u[group][...] + gx[group][xa] + (gx[group][xp] + gx[group][xm])
            for place, (pair, jb, ih) in enumerate(GROUPS[group]):
                rest[block_of(pair, jb, ih)] = summed[place]
            for pair, jb, ih in GROUPS[group]:
                if ih:
                    rest_copy(pair, jb, ih).start()
                    continue
                same = rest_home & (src_jb == jb)

                @pl.when(same)
                def _():
                    rest_in[pair, zl] = rest[block_of(pair, jb, ih)]

                @pl.when(jnp.logical_not(same))
                def _():
                    rest_copy(pair, jb, ih).start()

    def rest_receive(pair):
        @pl.when(zl == 1)
        def _():
            for part in range(2):

                @pl.when(jnp.logical_not(rest_home & (zl == part)))
                def _():
                    pltpu.make_async_remote_copy(
                        src_ref=rest.at[0],
                        dst_ref=rest_in.at[pair, part],
                        send_sem=r_send.at[0],
                        recv_sem=r_recv.at[pair, part],
                        device_id={"x": xp},
                        device_id_type=MESH,
                    ).wait_recv()

            fr[pair, 0, SENT[1] : PART] = rest_in[pair, 0] + rest_in[pair, 1]
            fr[pair, 1, SENT[1] : PART] = jnp.zeros((REST, WIDTH), F32)

    def deliver(pair):
        for way in range(2):
            yc[pair, way, 2].wait_recv()
            yc[pair, way, 3].wait_recv()
        done = total[pair, y] + (yr[pair, 0, 2] + yr[pair, 1, 2]) + (yr[pair, 0, 3] + yr[pair, 1, 3])
        for part in range(2):
            fs[pair, part, 0:STAT] = done[LEAD:ROWS]
            fs[pair, part, STAT : SENT[part]] = done[OWN:LEAD] if part else done[0:OWN]
            same = at_home & (zl == part)

            @pl.when(same)
            def _():
                fr[pair, zl, 0 : SENT[part]] = fs[pair, part, 0 : SENT[part]]

            @pl.when(jnp.logical_not(same))
            def _():
                final_copy(pair, part).start()

    def final_copy(pair, part):
        return pltpu.make_async_remote_copy(
            src_ref=fs.at[pair, part, 0 : SENT[part]],
            dst_ref=fr.at[pair, zl, 0 : SENT[part]],
            send_sem=f_send.at[pair, part],
            recv_sem=f_recv.at[pair, zl],
            device_id={"y": owner_y, "zl": part, "zh": owner_h, "core": half},
            device_id_type=MESH,
        )

    def receive(pair):
        for part in range(2):

            for own in range(2):

                @pl.when((zl == own) & jnp.logical_not(at_home & (zl == part)))
                def _():
                    pltpu.make_async_remote_copy(
                        src_ref=fs.at[pair, part, 0 : SENT[own]],
                        dst_ref=fr.at[pair, part, 0 : SENT[own]],
                        send_sem=f_send.at[pair, part],
                        recv_sem=f_recv.at[pair, part],
                        device_id={"x": xp},
                        device_id_type=MESH,
                    ).wait_recv()

        rest_receive(pair)
        both = fr[pair, 0] + fr[pair, 1]
        count = both[4 : 5, 0:1]
        lane = lax.broadcasted_iota(jnp.int32, (OWN, WIDTH), 1)
        row = lax.broadcasted_iota(jnp.int32, (OWN, WIDTH), 0)
        own = lane == row + (x * BLOCK + zl * OWN)

        def column(line):
            return jnp.sum(jnp.where(own, line, 0.0), axis=1, keepdims=True)

        mean_first = both[0:1] / count
        square_first = both[1 : 2] / count
        mean_second = column(both[2 : 3]) / count
        square_second = column(both[3 : 4]) / count
        spread_first = jnp.sqrt(square_first - mean_first * mean_first + EPS)
        spread_second = jnp.sqrt(square_second - mean_second * mean_second + EPS)
        out_ref[pair] = (both[STAT:PART] / count - mean_second * mean_first) / (spread_second * spread_first)

    def enter():
        owners = 4 * at_hub.astype(jnp.int32) - rest_home.astype(jnp.int32)
        pl.semaphore_wait(barrier, 12 - at_home.astype(jnp.int32) + owners)

    pick_first(0)
    enter()
    offer(0, "a")
    offer(0, "p")
    pick_second(0)
    offer(0, "b")
    offer(0, "s")
    arrive(0, "p")
    multiply(0, 0, 0)
    pick_first(1)
    offer(1, "a")
    offer(1, "p")
    pick_second(1)
    offer(1, "b")
    offer(1, "s")
    pass_on(0, 0, 0)
    arrive(1, "p")
    multiply(1, 0, 0)
    w_step(0, 0)
    collect(0, 0, 0)
    pass_on(1, 0, 0)
    forward(0)
    w_step(0, 1)
    arrive(0, "ap")
    multiply(0, 0, 1)
    arrive(0, "b", "s")
    multiply(0, 1, 1)
    collect(1, 0, 0)
    multiply(0, 1, 0)
    w_step(1, 0)
    pass_on(0, 0, 1)
    w_gather(0)
    pass_on(0, 1, 1)
    forward(1)
    pass_on(0, 1, 0)
    w_step(1, 1)
    arrive(1, "ap")
    multiply(1, 0, 1)
    arrive(1, "b", "s")
    multiply(1, 1, 0)
    multiply(1, 1, 1)
    w_deliver(0)
    collect(0, 0, 1)
    w_step(2, 0)
    collect(0, 1, 1)
    collect(0, 1, 0)
    y_step(0, 0)
    pass_on(1, 0, 1)
    w_gather(1)
    pass_on(1, 1, 0)
    pass_on(1, 1, 1)
    w_step(2, 1)
    collect(1, 0, 1)
    y_step(0, 1)
    w_deliver(1)
    collect(1, 1, 0)
    collect(1, 1, 1)
    y_step(1, 0)
    w_gather(2)
    deliver(0)
    y_step(1, 1)
    w_deliver(2)
    receive(0)
    deliver(1)
    receive(1)

    for copy in sent:
        copy.wait_send()
    for pair in range(PAIRS):
        for part in range(2):

            @pl.when(jnp.logical_not(at_home & (zl == part)))
            def _():
                final_copy(pair, part).wait_send()
    for group, blocks in enumerate(GROUPS):

        @pl.when(jnp.logical_not(at_hub))
        def _():
            gather_copy(group, x).wait_send()

        for pair, jb, ih in blocks:

            @pl.when(at_hub & jnp.logical_not(rest_home & (src_jb == jb) & (ih == 0)))
            def _():
                rest_copy(pair, jb, ih).wait_send()


def cross(pair_table, image, view, embeddings):
    blocks = 4 * PAIRS
    dma = pltpu.SemaphoreType.DMA
    vmem = pl.BlockSpec(memory_space=pltpu.VMEM)
    return pl.pallas_call(
        cross_kernel,
        out_shape=jax.ShapeDtypeStruct((PAIRS, OWN, WIDTH), F32),
        in_specs=[pl.BlockSpec(memory_space=pltpu.SMEM), vmem, vmem, pl.BlockSpec(memory_space=pl.ANY)],
        out_specs=vmem,
        scratch_shapes=[
            pltpu.VMEM((STEPS * SLOTS, WIDTH), BF16),
            pltpu.VMEM((IMG_DEV, WIDTH), F32),
            pltpu.VMEM((IMG_DEV, 128), F32),
            pltpu.VMEM((PAIRS, 1, WIDTH), F32),
            pltpu.VMEM((PAIRS, IMG_DEV, WIDTH), BF16),
            pltpu.VMEM((PAIRS, WIDTH, IMG_DEV), BF16),
            pltpu.VMEM((PAIRS, STAT, WIDTH), F32),
            pltpu.VMEM((PAIRS, IMG_DEV, WIDTH), BF16),
            pltpu.VMEM((PAIRS, IMG_DEV, WIDTH), BF16),
            pltpu.VMEM((PAIRS, IMG_DEV, WIDTH), BF16),
            pltpu.VMEM((PAIRS, WIDTH, IMG_DEV), BF16),
            pltpu.VMEM((PAIRS, STAT, WIDTH), F32),
            pltpu.VMEM((PAIRS, 2, 2, STAT, WIDTH), F32),
            pltpu.VMEM((blocks, NX, 2, ROWS, WIDTH), F32),
            pltpu.VMEM((blocks, ROWS, WIDTH), F32),
            pltpu.VMEM((blocks, ROWS, WIDTH), F32),
            pltpu.VMEM((blocks, 2, ROWS, WIDTH), F32),
            pltpu.VMEM((blocks, 2, ROWS, WIDTH), F32),
            pltpu.VMEM((PAIRS, NY, ROWS, WIDTH), F32),
            pltpu.VMEM((PAIRS, 2, 4, ROWS, WIDTH), F32),
            pltpu.VMEM((PAIRS, 2, PART, WIDTH), F32),
            pltpu.VMEM((PAIRS, 2, PART, WIDTH), F32),
            *(pltpu.VMEM((NY, len(blocks_of), REST, WIDTH), F32) for blocks_of in GROUPS),
            *(pltpu.VMEM((2, 4, len(blocks_of), REST, WIDTH), F32) for blocks_of in GROUPS),
            pltpu.VMEM((blocks, REST, WIDTH), F32),
            pltpu.VMEM((PAIRS, 2, REST, WIDTH), F32),
            *(pltpu.VMEM((len(blocks_of), REST, WIDTH), F32) for blocks_of in GROUPS),
            *(pltpu.VMEM((NX, len(blocks_of), REST, WIDTH), F32) for blocks_of in GROUPS),
            dma((STEPS,)),
            dma((PAIRS, 5)),
            dma((PAIRS, 5)),
            dma((blocks, 6)),
            dma((blocks, 6)),
            dma((PAIRS, 2, 4)),
            dma((PAIRS, 2, 4)),
            dma((PAIRS, 2)),
            dma((PAIRS, 2)),
            dma((len(GROUPS), 2, 4)),
            dma((len(GROUPS), 2, 4)),
            dma((blocks,)),
            dma((PAIRS, 2)),
            dma((len(GROUPS),)),
            dma((len(GROUPS), NX)),
        ],
        compiler_params=pltpu.CompilerParams(collective_id=0, has_side_effects=True),
        name="cross",
    )(pair_table, image, view, embeddings)


def local(embeddings, slot_image, slot_view, pair_table):
    shape = (STEPS * TILE, 128)
    block = cross(pair_table, slot_image.reshape(shape), slot_view.reshape(shape), embeddings)
    return jnp.swapaxes(block, 1, 2)


def solution(mesh):
    split = Mesh(mesh.devices.reshape(NY, NX, 2, 4, 2), AXES)
    placed = (P(DP, FEAT), P(DP), P(DP), P())
    return jax.shard_map(local, mesh=split, in_specs=placed, out_specs=P(None, FEAT, DP), check_vma=False)
```
